128 devices in a mesh: chan: 4 (over y), tm: 32 (over z, x, core).
Axes of the slice: x: 4, y: 4, z: 4, core: 2. Of those that a mesh axis runs over, the one named last changes fastest.
Arguments:
- strain: float32 [768, 524288], P('chan', 'tm'), may hold values from -6 to 6
Outputs:
- power: float32 [768, 8192], P('chan', 'tm')
- nyquist: float32 [768], P('chan')
- mean_power: float32 [8192], P('tm')
The draws below stay inside these ranges and needn't reach their ends.
All inputs are finite; a program needn't handle non-finite values.
Results may differ from the reference program's by a relative error of at most 0.00007.
Values sent between devices are 32-bit elements; how exact they have to be, the bound alone decides.
A program may use at most 192 MiB of HBM per device.

```python
import jax
import jax.numpy as jnp
from jax import lax

SEG = 16384
HOP = 8192
BINS = 8192
CHANNELS = 768
SAMPLES = 524288
SEGMENTS = 63


def level_of(stream_key, extent, split, low, top_value):
    loudness = 1.0
    for dim, shards_of in split:
        draws = jax.random.uniform(jax.random.fold_in(jax.random.fold_in(stream_key, 6), dim), (shards_of,), jnp.float32, low / len(split), top_value / len(split))
        loudness = loudness * jnp.repeat(jnp.exp(draws), extent[dim] // shards_of).reshape((-1,) + (1,) * (len(extent) - 1 - dim))
    return loudness


def bell_draw(key, dims, spread, most, cuts=(), kind=jnp.bfloat16):
    drawn = jax.random.normal(key, dims, jnp.float32) * spread
    if len(cuts) > 0:
        drawn = level_of(key, dims, cuts, -0.22, 0.18) * drawn
    return jnp.clip(drawn, min=-most, max=most).astype(kind)


def setup_inputs(seed: int = 0) -> dict:
    keys = jax.random.split(jax.random.key(seed), 2)
    strain = bell_draw(keys[0], (CHANNELS, SAMPLES), 1.0, 6.0, ((0, 4), (1, 32)), jnp.float32)
    return dict(strain=strain)


def hann_window():
    sample_pos = jnp.arange(SEG, dtype=jnp.float32)
    return 0.5 - 0.5 * jnp.cos(2.0 * jnp.pi * sample_pos / SEG)


def reference(strain):
    window = hann_window()
    energy = jnp.sum(window * window)

    def one_channel(signal):
        blocks = signal.reshape(SEGMENTS + 1, HOP)
        pieces = jnp.concatenate([blocks[:-1], blocks[1:]], axis=1)
        centred = (pieces - jnp.mean(pieces, axis=1, keepdims=True)) * window
        spectrum = jnp.fft.rfft(centred, axis=1)
        return jnp.sum(jnp.real(spectrum) ** 2 + jnp.imag(spectrum) ** 2, axis=0)

    totals = lax.map(one_channel, strain)
    doubling = jnp.where(jnp.arange(BINS) == 0, 1.0, 2.0).astype(totals.dtype)
    power = totals[:, :BINS] * doubling / (SEGMENTS * energy)
    nyquist = totals[:, BINS] / (SEGMENTS * energy)
    mean_power = jnp.mean(power, axis=0)
    return power, nyquist, mean_power
```

```python
import functools

import jax
import jax.numpy as jnp
import numpy as np
from jax import lax
from jax.experimental import pallas as pl
from jax.experimental.pallas import tpu as pltpu
from jax.sharding import PartitionSpec as P

SEG = 16384
ROOT = 128
F32 = jnp.float32
BF16 = jnp.bfloat16
STRIDE = 8
CHUNK = 2


def split(values):
    high = values.astype(BF16)
    low = (values - high.astype(F32)).astype(BF16)
    return high, low


def split_np(values):
    high = values.astype(np.float32).astype(BF16)
    low = (values - high.astype(np.float64)).astype(np.float32).astype(BF16)
    return high, low


def lane_bins():
    lane = np.arange(ROOT)
    owner, part = lane // 4, lane % 4
    return np.where(part < 2, 2 * owner + part, 127 - 2 * owner - (part - 2))


def tables():
    turn = 2.0 * np.pi / ROOT
    a = np.arange(ROOT)
    k1 = np.arange(64)
    cos_rows = np.cos(turn * ((k1[:, None] * a) % ROOT))
    sin_rows = -np.sin(turn * ((k1[:, None] * a) % ROOT))
    sin_rows[0] = 1.0 - 2.0 * (a % 2)
    first = np.concatenate([cos_rows, sin_rows], 0)
    first_high, first_low = split_np(first)
    first_high = np.concatenate([first_high, first_high], 1)
    first_low = np.concatenate([first_low, first_low], 1)
    q = lane_bins()
    cos_q = np.cos(turn * ((a[:, None] * q) % ROOT))
    sin_q = np.sin(turn * ((a[:, None] * q) % ROOT))
    last = np.concatenate(
        [np.concatenate([cos_q, -sin_q], 1), np.concatenate([sin_q, cos_q], 1)], 0
    )
    last_high, last_low = split_np(last)
    long_turn = 2.0 * np.pi / SEG
    twist = long_turn * (k1[:, None] * a)
    cos_twist = np.cos(twist).astype(np.float32)
    sin_twist = np.sin(twist).astype(np.float32)
    mid = long_turn * 64 * a
    mid_twist = np.stack([np.cos(mid), np.sin(mid)] + [0 * mid] * 6).astype(np.float32)
    n = np.arange(SEG, dtype=np.float64)
    window = (0.5 - 0.5 * np.cos(2.0 * np.pi * n / SEG)).astype(np.float32)
    slot, kind, k = np.meshgrid(np.arange(2), np.arange(2), np.arange(64), indexing="ij")
    place = np.where(slot == 0, k, np.where(k == 0, 64, 128 - k)) + 128 * kind
    perm = np.zeros((256, 256), np.float32)
    perm[np.arange(256), place.reshape(-1)] = 1.0
    energy = float(np.sum(window.astype(np.float64) ** 2))
    return (
        [
            np.concatenate([first_high, first_low], 0),
            last_high,
            last_low,
            cos_twist,
            sin_twist,
            mid_twist,
            window.reshape(ROOT, ROOT),
            perm.astype(BF16),
        ],
        energy,
    )


def dot(a, b):
    return jnp.dot(a, b, preferred_element_type=F32)


def first_stage(blocks, start, segs, ch, tabs, mean_ref, mean_base, mid_ref, high_ref, low_ref, row0):
    t_ref, vh_ref, vl_ref, c_ref, s_ref, mid_tw, w_ref = tabs
    w0, w1 = w_ref[:64, :], w_ref[64:, :]
    row = lax.broadcasted_iota(jnp.int32, (8, 256), 0)
    for pair in range(segs // 2):
        highs, lows = [], []
        for s in (2 * pair, 2 * pair + 1):
            mean = mean_ref[pl.ds(mean_base + s * 8 + ch, 1), :]
            r0, b0, b1 = blocks, start + s * 512, start + s * 512 + 512
            x0 = (r0[pl.ds(b0 + ch, 64, STRIDE), :] - mean) * w0
            x1 = (r0[pl.ds(b1 + ch, 64, STRIDE), :] - mean) * w1
            high, low = split(jnp.concatenate([x0, x1], 0))
            highs.append(high)
            lows.append(low)
        x = jnp.concatenate(
            [jnp.concatenate(highs, 1), jnp.concatenate(lows, 1)], 0
        )
        both = dot(t_ref[...], x)
        d = both[:128] + both[128:]
        fr = d[:64]
        fi = jnp.concatenate([jnp.where(row == 0, 0.0, d[64:72]), d[72:]], 0)
        mid = d[64:65]
        c, s_ = c_ref[...], s_ref[...]
        for i in range(2):
            s = 2 * pair + i
            lanes = slice(i * ROOT, (i + 1) * ROOT)
            tr = fr[:, lanes] * c + fi[:, lanes] * s_
            ti = fi[:, lanes] * c - fr[:, lanes] * s_
            put = row0 + 64 * s
            high, low = split(jnp.concatenate([tr, ti], 1))
            high_ref[pl.ds(put, 64), :] = high
            low_ref[pl.ds(put, 64), :] = low
            m = mid[:, lanes]
            mid_ref[pl.ds(mean_base + s * 8 + ch, 1), :] = jnp.concatenate(
                [m * mid_tw[0:1, :], -m * mid_tw[1:2, :]], 1
            )


def squares(high, low, vh_ref, vl_ref):
    o = dot(high, vh_ref[...]) + dot(low, vh_ref[...]) + dot(high, vl_ref[...])
    return o[:, :ROOT] * o[:, :ROOT] + o[:, ROOT:] * o[:, ROOT:]


GROUPS = 6
HALF_ROWS = 512
ENTRY_ROWS = 5 * HALF_ROWS
SEGS = 4


def remote(src, dst, send, recv, axis, index):
    return pltpu.make_async_remote_copy(
        src_ref=src,
        dst_ref=dst,
        send_sem=send,
        recv_sem=recv,
        device_id={axis: index},
        device_id_type=pl.DeviceIdType.MESH,
    )


def twin(r):
    return r + 1 - 2 * lax.rem(r, 2)


def welch_kernel(scale, x_ref, *refs):
    tabs, perm_ref, refs = refs[:7], refs[7], refs[8:]
    power_out, edge_out, mean_out = refs[:3]
    (buf, mean_ref, mid_ref, high_ref, low_ref, pow_ref, zs, zr, xs, xr, allf) = refs[3:14]
    (edge_z, edge_x, edge_sum, mean_buf) = refs[14:18]
    (load_sem, pair_send, pair_recv, halo_send, halo_recv, z_send, z_recv) = refs[18:25]
    (x_send, x_recv, d_send, d_recv, e_send, e_recv, m_send, m_recv) = refs[25:]
    y = lax.axis_index("chan")
    t = lax.axis_index("tm")
    core = lax.rem(t, 2)
    chip = t // 2
    x = lax.rem(chip, 4)
    z = chip // 4
    other = 1 - core
    device = lambda zz, xx, cc: (zz * 4 + xx) * 2 + cc

    def entry(g, half):
        return (g * 2 + half) * ENTRY_ROWS

    def load(g, half):
        row = (12 * core + 6 * half + g) * 1024
        to = entry(g, half) + (2 * core + half) * HALF_ROWS
        return pltpu.make_async_copy(
            x_ref.at[pl.ds(row, 1024), :], buf.at[pl.ds(to, 1024), :], load_sem.at[g, half]
        )

    def pair(g, half):
        row = (12 * other + 6 * half + g) * 1024
        to = entry(g, half) + (2 * core + half) * HALF_ROWS
        return remote(
            x_ref.at[pl.ds(row, 1024), :],
            buf.at[pl.ds(to, 1024), :],
            pair_send.at[g, half],
            pair_recv.at[g, half],
            "tm",
            device(z, x, other),
        )

    def halo(g, h):
        row = (12 * h + 6 * core + g) * 1024 + core * HALF_ROWS
        to = entry(g, core) + other * 4 * HALF_ROWS
        target = lax.rem(chip + 2 * core - 1 + 16, 16)
        return remote(
            x_ref.at[pl.ds(row, HALF_ROWS), :],
            buf.at[pl.ds(to, HALF_ROWS), :],
            halo_send.at[g, h],
            halo_recv.at[g, core],
            "tm",
            target * 2 + h,
        )

    def halo_arrival(g, half):
        to = entry(g, half) + (1 - half) * 4 * HALF_ROWS
        return remote(
            x_ref.at[pl.ds(0, HALF_ROWS), :],
            buf.at[pl.ds(to, HALF_ROWS), :],
            halo_send.at[g, half],
            halo_recv.at[g, half],
            "tm",
            device(z, x, other),
        )

    def partners(r, way):
        if way == 0:
            return twin(r), 3 - r
        return 3 - r, twin(r)

    def z_copy(g, way, slot):
        near, far = partners(z, way)
        to = near if slot < 2 else far
        chunk = (near, partners(near, way)[1], far)[slot]
        return remote(
            zs.at[way, g, pl.ds(chunk * 32, 32), :],
            zr.at[way, g, slot],
            z_send.at[way, g, slot],
            z_recv.at[way, g, slot],
            "tm",
            device(to, x, core),
        )

    def x_copy(g, way, slot):
        near, far = partners(x, way)
        to = near if slot < 2 else far
        chunk = (near, partners(near, way)[1], far)[slot]
        return remote(
            xs.at[way, g, pl.ds(chunk * 8, 8), :],
            xr.at[way, g, slot],
            x_send.at[way, g, slot],
            x_recv.at[way, g, slot],
            "tm",
            device(z, to, core),
        )

    def d_copy(g, half_owner):
        rows = allf.at[half_owner, pl.ds(g * 64, 64), :]
        return remote(rows, rows, d_send.at[g], d_recv.at[g], "tm", device(z, x, other))

    def edge_copy(stage, step):
        if stage == 0:
            return remote(
                edge_z.at[0], edge_z.at[step], e_send.at[0, step], e_recv.at[0, step],
                "tm", device(lax.rem(z + step, 4), x, core),
            )
        if stage == 1:
            return remote(
                edge_x.at[0], edge_x.at[step], e_send.at[1, step], e_recv.at[1, step],
                "tm", device(z, lax.rem(x + step, 4), core),
            )
        return remote(
            edge_sum.at[0], edge_sum.at[1], e_send.at[2, 0], e_recv.at[2, 0],
            "tm", device(z, x, other),
        )

    def mean_copy(step):
        return remote(
            mean_buf.at[0], mean_buf.at[step], m_send.at[step], m_recv.at[step],
            "chan", lax.rem(y + step, 4),
        )

    def z_first(g):
        for slot in (1, 0):
            for way in range(2):
                z_copy(g, way, slot).start()

    def z_second(g):
        for way in range(2):
            far = partners(z, way)[1]
            z_copy(g, way, 1).wait_recv()
            rows = pl.ds(pl.multiple_of(far * 32, 32), 32)
            zs[way, g, rows, :] = zs[way, g, rows, :] + zr[way, g, 1]
            z_copy(g, way, 2).start()

    def x_first(g):
        for way in range(2):
            z_copy(g, way, 0).wait_recv()
            z_copy(g, way, 2).wait_recv()
            rows = pl.ds(pl.multiple_of(z * 32, 32), 32)
            xs[way, g] = zs[way, g, rows, :] + zr[way, g, 0] + zr[way, g, 2]
            x_copy(g, way, 1).start()
            x_copy(g, way, 0).start()

    def x_second(g):
        for way in range(2):
            far = partners(x, way)[1]
            x_copy(g, way, 1).wait_recv()
            rows = pl.ds(pl.multiple_of(far * 8, 8), 8)
            xs[way, g, rows, :] = xs[way, g, rows, :] + xr[way, g, 1]
            x_copy(g, way, 2).start()

    def to_pair(g):
        for way in range(2):
            x_copy(g, way, 0).wait_recv()
            x_copy(g, way, 2).wait_recv()
            rows = pl.ds(pl.multiple_of(x * 8, 8), 8)
            total = xs[way, g, rows, :] + xr[way, g, 0] + xr[way, g, 2]
            for i in range(4):
                at = pl.multiple_of(g * 64 + (way * 4 + i) * 8, 8)
                allf[core, pl.ds(at, 8), :] = total[:, i * ROOT : (i + 1) * ROOT]
        d_copy(g, core).start()

    lane = lax.broadcasted_iota(jnp.int32, (8, ROOT), 1)

    def compute(g):
        for half in range(2):
            load(g, half).wait()
            first = pl.multiple_of(entry(g, half), 8)
            pair_arrival(g, half).wait_recv()
            halo_arrival(g, half).wait_recv()
            sums = []
            for i in range(5):
                rows = buf[pl.ds(pl.multiple_of(first + i * HALF_ROWS, 8), HALF_ROWS), :]
                rows = rows.reshape(64, 8, ROOT)
                sums.append(jnp.sum(jnp.sum(rows, axis=0), axis=1, keepdims=True))
            base = half * 32
            for s in range(SEGS):
                mean = (sums[s] + sums[s + 1]) * (1.0 / SEG)
                mean_ref[base + s * 8 : base + s * 8 + 8, :] = jnp.broadcast_to(mean, (8, ROOT))
            absent = (chip == 15, 3) if half == 0 else (chip == 0, 0)
            for ch in range(8):
                first_stage(
                    buf, first, SEGS, ch, tabs, mean_ref, base, mid_ref, high_ref, low_ref, ch * 256
                )
            for c0 in range(0, 8, CHUNK):
                sl = slice(c0 * 256, (c0 + CHUNK) * 256)
                sq = squares(high_ref[sl, :], low_ref[sl, :], tabs[1], tabs[2])
                for ch in range(c0, c0 + CHUNK):
                    power = jnp.zeros((64, ROOT), F32)
                    for s in range(SEGS):
                        r = (ch - c0) * 256 + s * 64
                        sqs = sq[r : r + 64]
                        if s == absent[1]:
                            sqs = jnp.where(absent[0], 0.0, sqs)
                        power = power + sqs
                    at = ch * 128 + 64 * half
                    pow_ref[at : at + 64, :] = power
            sq = squares(*split(mid_ref[base : base + 32, :]), tabs[1], tabs[2])
            middle = jnp.zeros((8, ROOT), F32)
            for s in range(SEGS):
                sqs = sq[s * 8 : s * 8 + 8]
                if s == absent[1]:
                    sqs = jnp.where(absent[0], 0.0, sqs)
                middle = middle + sqs
            zero = pow_ref[pl.ds(64 * half, 8, 128), :]
            last = jnp.sum(jnp.where(lane == ROOT - 1, zero, 0.0), axis=1, keepdims=True)
            rows = slice(half * 8, half * 8 + 8)
            edge_z[0, rows, :] = jnp.where(
                lane == g, jnp.broadcast_to(last, (8, ROOT)), edge_z[0, rows, :]
            )
            pow_ref[pl.ds(64 * half, 8, 128), :] = jnp.where(lax.rem(lane, 4) >= 2, middle, zero)
        for i in range(8):
            block = pow_ref[i * 128 : (i + 1) * 128, :].T
            zs[i // 4, g, :, (i % 4) * ROOT : (i % 4 + 1) * ROOT] = block

    def pair_arrival(g, half):
        to = entry(g, half) + (2 * other + half) * HALF_ROWS
        return remote(
            x_ref.at[pl.ds(0, 1024), :],
            buf.at[pl.ds(to, 1024), :],
            pair_send.at[g, half],
            pair_recv.at[g, half],
            "tm",
            device(z, x, other),
        )

    for g in range(GROUPS):
        for half in range(2):
            load(g, half).start()
    barrier = pltpu.get_barrier_semaphore()
    peers = [("tm", device(z, x, other))]
    for step in (1, 15):
        for h in range(2):
            peers.append(("tm", lax.rem(chip + step, 16) * 2 + h))
    for step in (1, 2, 3):
        peers.append(("tm", device(lax.rem(z + step, 4), x, core)))
        peers.append(("tm", device(z, lax.rem(x + step, 4), core)))
        peers.append(("chan", lax.rem(y + step, 4)))
    for axis, index in peers:
        pl.semaphore_signal(
            barrier, inc=1, device_id={axis: index}, device_id_type=pl.DeviceIdType.MESH
        )
    pl.semaphore_wait(barrier, len(peers))
    for g in range(GROUPS):
        for half in range(2):
            pair(g, half).start()
        for h in range(2):
            halo(g, h).start()
    edge_z[0] = jnp.zeros((16, ROOT), F32)

    def step(g, carry):
        @pl.when(g < GROUPS)
        def _():
            compute(g)
            z_first(g)

        @pl.when(g == GROUPS - 1)
        def _():
            for s in (1, 2, 3):
                edge_copy(0, s).start()

        @pl.when((g >= 1) & (g < GROUPS + 1))
        def _():
            z_second(g - 1)

        @pl.when((g >= 2) & (g < GROUPS + 2))
        def _():
            x_first(g - 2)

        @pl.when((g >= 3) & (g < GROUPS + 3))
        def _():
            x_second(g - 3)

        @pl.when(g >= 4)
        def _():
            to_pair(g - 4)

        return carry

    lax.fori_loop(0, GROUPS + 4, step, 0)

    total = edge_z[0]
    for s in (1, 2, 3):
        edge_copy(0, s).wait_recv()
        total = total + edge_z[s]
    edge_x[0] = total
    for s in (1, 2, 3):
        edge_copy(1, s).start()

    for g in range(GROUPS):
        d_copy(g, other).wait_recv()
    lane_row = lax.broadcasted_iota(jnp.int32, (1, ROOT), 1)
    column = jnp.zeros((8, 256), F32)
    pieces = []
    for par in range(2):
        stacked = []
        for h in range(2):
            near = allf[h, pl.ds(4 * core + par, 48, 8), :]
            far = allf[h, pl.ds(4 * core + par + 2, 48, 8), :]
            stacked.append(jnp.concatenate([near, far], 1))
        value = jnp.concatenate(stacked, 0)
        high, rest = split(value)
        low = rest.astype(F32)
        rest = (value - high.astype(F32)) - low
        placed = dot(high, perm_ref[...]) + dot(low.astype(BF16), perm_ref[...])
        placed = placed + dot(rest.astype(BF16), perm_ref[...])
        factor = jnp.full((1, ROOT), 2.0 * scale, F32)
        if par == 0:
            factor = jnp.where((lane_row == 0) & (t == 0), scale, factor)
        for kind in range(2):
            out = placed[:, kind * ROOT : (kind + 1) * ROOT] * factor
            for h in range(2):
                at = h * 96 + kind * 48
                power_out[at : at + 48, par * ROOT : (par + 1) * ROOT] = out[h * 48 : h * 48 + 48]
            pieces.append(out)
    sums = []
    for par in range(2):
        both = pieces[2 * par] + pieces[2 * par + 1]
        sums.append(jnp.sum(both, axis=0, keepdims=True))
    mean_buf[0] = jnp.broadcast_to(jnp.concatenate(sums, 1), (8, 256))
    for s in (1, 2, 3):
        mean_copy(s).start()

    total = edge_x[0]
    for s in (1, 2, 3):
        edge_copy(1, s).wait_recv()
        total = total + edge_x[s]
    edge_sum[0] = total
    edge_copy(2, 0).start()

    def drain(g, carry):
        for way in range(2):
            for slot in range(3):
                z_copy(g, way, slot).wait_send()
                x_copy(g, way, slot).wait_send()
            pair(g, way).wait_send()
            halo(g, way).wait_send()
        d_copy(g, core).wait_send()
        return carry

    lax.fori_loop(0, GROUPS, drain, 0)
    for s in (1, 2, 3):
        edge_copy(0, s).wait_send()
        edge_copy(1, s).wait_send()
    edge_copy(2, 0).wait_recv()
    edge_copy(2, 0).wait_send()
    edge_out[core] = edge_sum[0] * scale
    edge_out[other] = edge_sum[1] * scale
    mean = mean_buf[0]
    for s in (1, 2, 3):
        mean_copy(s).wait_recv()
        mean = mean + mean_buf[s]
    mean_out[...] = mean * (1.0 / 768.0)
    for s in (1, 2, 3):
        mean_copy(s).wait_send()


def per_device(strain):
    rows = strain.shape[0]
    tabs_np, energy = tables()
    tabs = [jnp.asarray(t) for t in tabs_np]
    groups = rows // 8
    x4 = strain.reshape(groups, 8, ROOT, ROOT).transpose(0, 2, 1, 3)
    x2 = x4.reshape(groups * 1024, ROOT)
    vmem = pl.BlockSpec(memory_space=pltpu.VMEM)
    dma = pltpu.SemaphoreType.DMA
    power, edge, mean = pl.pallas_call(
        functools.partial(welch_kernel, 1.0 / (63.0 * energy)),
        out_shape=[
            jax.ShapeDtypeStruct((192, 256), F32),
            jax.ShapeDtypeStruct((2, 16, ROOT), F32),
            jax.ShapeDtypeStruct((8, 256), F32),
        ],
        in_specs=[pl.BlockSpec(memory_space=pl.ANY)] + [vmem] * len(tabs),
        out_specs=[vmem] * 3,
        scratch_shapes=[
            pltpu.VMEM((GROUPS * 2 * ENTRY_ROWS, ROOT), F32),
            pltpu.VMEM((64, ROOT), F32),
            pltpu.VMEM((64, 256), F32),
            pltpu.VMEM((2048, 256), BF16),
            pltpu.VMEM((2048, 256), BF16),
            pltpu.VMEM((1024, ROOT), F32),
            pltpu.VMEM((2, GROUPS, 128, 512), F32),
            pltpu.VMEM((2, GROUPS, 3, 32, 512), F32),
            pltpu.VMEM((2, GROUPS, 32, 512), F32),
            pltpu.VMEM((2, GROUPS, 3, 8, 512), F32),
            pltpu.VMEM((2, GROUPS * 64, ROOT), F32),
            pltpu.VMEM((4, 16, ROOT), F32),
            pltpu.VMEM((4, 16, ROOT), F32),
            pltpu.VMEM((2, 16, ROOT), F32),
            pltpu.VMEM((4, 8, 256), F32),
            dma((GROUPS, 2)),
            dma((GROUPS, 2)),
            dma((GROUPS, 2)),
            dma((GROUPS, 2)),
            dma((GROUPS, 2)),
            dma((2, GROUPS, 3)),
            dma((2, GROUPS, 3)),
            dma((2, GROUPS, 3)),
            dma((2, GROUPS, 3)),
            dma((GROUPS,)),
            dma((GROUPS,)),
            dma((3, 4)),
            dma((3, 4)),
            dma((4,)),
            dma((4,)),
        ],
        compiler_params=pltpu.CompilerParams(
            collective_id=0, has_side_effects=True, vmem_limit_bytes=60 * 1024 * 1024
        ),
    )(x2, *tabs)
    nyquist = edge.reshape(2, 2, 8, ROOT)[..., :GROUPS].transpose(0, 1, 3, 2).reshape(rows)
    return power, nyquist, mean[0]


def solution(mesh):
    return jax.shard_map(
        per_device,
        mesh=mesh,
        in_specs=(P("chan", "tm"),),
        out_specs=(P("chan", "tm"), P("chan"), P("tm")),
        check_vma=False,
    )
```

```python
import functools

import jax
import jax.numpy as jnp
import numpy as np
from jax import lax
from jax.experimental import pallas as pl
from jax.experimental.pallas import tpu as pltpu
from jax.sharding import PartitionSpec as P

SEG = 16384
ROOT = 128
F32 = jnp.float32
BF16 = jnp.bfloat16
STRIDE = 8
CHUNK = 2


def split(values):
    high = values.astype(BF16)
    low = (values - high.astype(F32)).astype(BF16)
    return high, low


def split_np(values):
    high = values.astype(np.float32).astype(BF16)
    low = (values - high.astype(np.float64)).astype(np.float32).astype(BF16)
    return high, low


def lane_bins():
    lane = np.arange(ROOT)
    owner, part = lane // 4, lane % 4
    return np.where(part < 2, 2 * owner + part, 127 - 2 * owner - (part - 2))


def tables():
    turn = 2.0 * np.pi / ROOT
    a = np.arange(ROOT)
    k1 = np.arange(64)
    cos_rows = np.cos(turn * ((k1[:, None] * a) % ROOT))
    sin_rows = -np.sin(turn * ((k1[:, None] * a) % ROOT))
    sin_rows[0] = 1.0 - 2.0 * (a % 2)
    first = np.concatenate([cos_rows, sin_rows], 0)
    first_high, first_low = split_np(first)
    first_high = np.concatenate([first_high, first_high], 1)
    first_low = np.concatenate([first_low, first_low], 1)
    q = lane_bins()
    cos_q = np.cos(turn * ((a[:, None] * q) % ROOT))
    sin_q = np.sin(turn * ((a[:, None] * q) % ROOT))
    last = np.concatenate(
        [np.concatenate([cos_q, -sin_q], 1), np.concatenate([sin_q, cos_q], 1)], 0
    )
    last_high, last_low = split_np(last)
    long_turn = 2.0 * np.pi / SEG
    twist = long_turn * (k1[:, None] * a)
    cos_twist = np.cos(twist).astype(np.float32)
    sin_twist = np.sin(twist).astype(np.float32)
    mid = long_turn * 64 * a
    mid_twist = np.stack([np.cos(mid), np.sin(mid)] + [0 * mid] * 6).astype(np.float32)
    n = np.arange(SEG, dtype=np.float64)
    window = (0.5 - 0.5 * np.cos(2.0 * np.pi * n / SEG)).astype(np.float32)
    slot, kind, k = np.meshgrid(np.arange(2), np.arange(2), np.arange(64), indexing="ij")
    place = np.where(slot == 0, k, np.where(k == 0, 64, 128 - k)) + 128 * kind
    perm = np.zeros((256, 256), np.float32)
    perm[np.arange(256), place.reshape(-1)] = 1.0
    energy = float(np.sum(window.astype(np.float64) ** 2))
    return (
        [
            np.concatenate([first_high, first_low], 0),
            last_high,
            last_low,
            cos_twist,
            sin_twist,
            mid_twist,
            window.reshape(ROOT, ROOT),
            perm.astype(BF16),
        ],
        energy,
    )


def dot(a, b):
    return jnp.dot(a, b, preferred_element_type=F32)


def first_stage(blocks, start, segs, ch, tabs, mean_ref, mean_base, mid_ref, high_ref, low_ref, row0):
    t_ref, vh_ref, vl_ref, c_ref, s_ref, mid_tw, w_ref = tabs
    w0, w1 = w_ref[:64, :], w_ref[64:, :]
    row = lax.broadcasted_iota(jnp.int32, (8, 256), 0)
    for pair in range(segs // 2):
        highs, lows = [], []
        for s in (2 * pair, 2 * pair + 1):
            mean = mean_ref[pl.ds(mean_base + s * 8 + ch, 1), :]
            r0, b0, b1 = blocks, start + s * 512, start + s * 512 + 512
            x0 = (r0[pl.ds(b0 + ch, 64, STRIDE), :] - mean) * w0
            x1 = (r0[pl.ds(b1 + ch, 64, STRIDE), :] - mean) * w1
            high, low = split(jnp.concatenate([x0, x1], 0))
            highs.append(high)
            lows.append(low)
        x = jnp.concatenate(
            [jnp.concatenate(highs, 1), jnp.concatenate(lows, 1)], 0
        )
        both = dot(t_ref[...], x)
        d = both[:128] + both[128:]
        fr = d[:64]
        fi = jnp.concatenate([jnp.where(row == 0, 0.0, d[64:72]), d[72:]], 0)
        mid = d[64:65]
        c, s_ = c_ref[...], s_ref[...]
        for i in range(2):
            s = 2 * pair + i
            lanes = slice(i * ROOT, (i + 1) * ROOT)
            tr = fr[:, lanes] * c + fi[:, lanes] * s_
            ti = fi[:, lanes] * c - fr[:, lanes] * s_
            put = row0 + 64 * s
            high, low = split(jnp.concatenate([tr, ti], 1))
            high_ref[pl.ds(put, 64), :] = high
            low_ref[pl.ds(put, 64), :] = low
            m = mid[:, lanes]
            mid_ref[pl.ds(mean_base + s * 8 + ch, 1), :] = jnp.concatenate(
                [m * mid_tw[0:1, :], -m * mid_tw[1:2, :]], 1
            )


def squares(high, low, vh_ref, vl_ref):
    o = dot(high, vh_ref[...]) + dot(low, vh_ref[...]) + dot(high, vl_ref[...])
    return o[:, :ROOT] * o[:, :ROOT] + o[:, ROOT:] * o[:, ROOT:]


GROUPS = 6
HALF_ROWS = 512
ENTRY_ROWS = 5 * HALF_ROWS
SEGS = 4
BATCHES = 3
AHEAD = 2


def remote(src, dst, send, recv, axis, index):
    return pltpu.make_async_remote_copy(
        src_ref=src,
        dst_ref=dst,
        send_sem=send,
        recv_sem=recv,
        device_id={axis: index},
        device_id_type=pl.DeviceIdType.MESH,
    )


def twin(r):
    return r + 1 - 2 * lax.rem(r, 2)


def partners(r, way):
    if way == 0:
        return twin(r), 3 - r
    return 3 - r, twin(r)


def place(r, way):
    if way == 0:
        return lax.rem(2 * r - r // 2, 4)
    return r


def keep(r, way):
    return place(r, way) // 2 * 2


def welch_kernel(scale, x_ref, *refs):
    tabs, perm_ref, refs = refs[:7], refs[7], refs[8:]
    power_out, edge_out, mean_out = refs[:3]
    (relay, relay_send, relay_recv), refs = refs[3:6], refs[:3] + refs[6:]
    (buf, mean_ref, mid_ref, high_ref, low_ref, pow_ref) = refs[3:9]
    (zs, z_near, z_far, xs, x_near, x_far, allf) = refs[9:16]
    (edge_z, edge_x, edge_sum, mean_buf) = refs[16:20]
    (load_sem, pair_send, pair_recv, halo_send, halo_recv, z_send, z_recv) = refs[20:27]
    (x_send, x_recv, d_send, d_recv, e_send, e_recv, m_send, m_recv) = refs[27:]
    y = lax.axis_index("chan")
    t = lax.axis_index("tm")
    core = lax.rem(t, 2)
    chip = t // 2
    x = lax.rem(chip, 4)
    z = chip // 4
    other = 1 - core
    device = lambda zz, xx, cc: (zz * 4 + xx) * 2 + cc

    def entry(g, half):
        return (g * 2 + half) * ENTRY_ROWS

    def load(g, half):
        row = (12 * core + 6 * half + g) * 1024
        to = entry(g, half) + (2 * core + half) * HALF_ROWS
        return pltpu.make_async_copy(
            x_ref.at[pl.ds(row, 1024), :], buf.at[pl.ds(to, 1024), :], load_sem.at[g, half]
        )

    def pair(g, half):
        row = (12 * other + 6 * half + g) * 1024
        to = entry(g, half) + (2 * core + half) * HALF_ROWS
        return remote(
            x_ref.at[pl.ds(row, 1024), :],
            buf.at[pl.ds(to, 1024), :],
            pair_send.at[g, half],
            pair_recv.at[g, half],
            "tm",
            device(z, x, other),
        )

    def halo(g, half):
        there = entry(g, half) + (1 - half) * 4 * HALF_ROWS
        here = entry(g, half) + half * 4 * HALF_ROWS
        target = lax.rem(chip + (15 if half == 0 else 1), 16)
        return remote(
            buf.at[pl.ds(here, HALF_ROWS), :],
            buf.at[pl.ds(there, HALF_ROWS), :],
            halo_send.at[g, half],
            halo_recv.at[g, half],
            "tm",
            target * 2 + core,
        )

    def hop(g, half):
        here = entry(g, half) + half * 4 * HALF_ROWS
        return remote(
            buf.at[pl.ds(here, HALF_ROWS), :],
            relay.at[pl.ds(g * HALF_ROWS, HALF_ROWS), :],
            halo_send.at[g, half],
            relay_recv.at[g],
            "tm",
            device(lax.rem(z + (3 if half == 0 else 1), 4), x, core),
        )

    def onward(g):
        half = x // 3
        there = entry(g, half) + (1 - half) * 4 * HALF_ROWS
        return remote(
            relay.at[pl.ds(g * HALF_ROWS, HALF_ROWS), :],
            buf.at[pl.ds(there, HALF_ROWS), :],
            relay_send.at[g],
            halo_recv.at[g, half],
            "tm",
            device(z, 3 - x, core),
        )

    relays = (core == 1) & ((x == 0) | (x == 3))

    def z_copy(g, way, step):
        near, far = partners(z, way)
        if step == 0:
            start, rows, into, to = (2 - keep(z, way)) * 32, 64, z_near, near
        else:
            start, rows, into, to = place(far, way) * 32, 32, z_far, far
        return remote(
            zs.at[way, g, pl.ds(start, rows), :],
            into.at[way, g],
            z_send.at[way, g, step],
            z_recv.at[way, g, step],
            "tm",
            device(to, x, core),
        )

    def x_copy(b, way, step):
        near, far = partners(x, way)
        if step == 0:
            start, size, into, to = 2 - keep(x, way), 2, x_near, near
        else:
            start, size, into, to = place(far, way), 1, x_far, far
        return remote(
            xs.at[way, b, pl.ds(start, size)],
            into.at[way, b],
            x_send.at[way, b, step],
            x_recv.at[way, b, step],
            "tm",
            device(z, to, core),
        )

    def d_copy(b, half_owner):
        rows = allf.at[half_owner, pl.ds(b * 128, 128), :]
        return remote(rows, rows, d_send.at[b], d_recv.at[b], "tm", device(z, x, other))

    def edge_copy(stage, step):
        if stage == 0:
            return remote(
                edge_z.at[0], edge_z.at[step], e_send.at[0, step], e_recv.at[0, step],
                "tm", device(lax.rem(z + step, 4), x, core),
            )
        if stage == 1:
            return remote(
                edge_x.at[0], edge_x.at[step], e_send.at[1, step], e_recv.at[1, step],
                "tm", device(z, lax.rem(x + step, 4), core),
            )
        return remote(
            edge_sum.at[0], edge_sum.at[1], e_send.at[2, 0], e_recv.at[2, 0],
            "tm", device(z, x, other),
        )

    def mean_copy(step):
        return remote(
            mean_buf.at[0], mean_buf.at[step], m_send.at[step], m_recv.at[step],
            "chan", lax.rem(y + step, 4),
        )

    def z_first(g):
        for way in range(2):
            z_copy(g, way, 0).start()

    def z_second(g):
        for way in range(2):
            far = partners(z, way)[1]
            z_copy(g, way, 0).wait_recv()
            at = place(far, way)
            rows = pl.ds(pl.multiple_of(at * 32, 32), 32)
            got = pl.ds(pl.multiple_of((at - keep(z, way)) * 32, 32), 32)
            zs[way, g, rows, :] = zs[way, g, rows, :] + z_near[way, g, got, :]
            z_copy(g, way, 1).start()

    def z_last(g):
        for way in range(2):
            z_copy(g, way, 1).wait_recv()
            at = place(z, way)
            rows = pl.ds(pl.multiple_of(at * 32, 32), 32)
            got = pl.ds(pl.multiple_of((at - keep(z, way)) * 32, 32), 32)
            total = zs[way, g, rows, :] + z_near[way, g, got, :] + z_far[way, g]
            for chunk in range(4):
                spot = (0, 2, 3, 1)[chunk] if way == 0 else chunk
                xs[way, g // 2, spot, lax.rem(g, 2)] = total[chunk * 8 : chunk * 8 + 8, :]

    def x_first(b):
        for way in range(2):
            x_copy(b, way, 0).start()

    def x_second(b):
        for way in range(2):
            far = partners(x, way)[1]
            x_copy(b, way, 0).wait_recv()
            at = place(far, way)
            xs[way, b, at] = xs[way, b, at] + x_near[way, b, at - keep(x, way)]
            x_copy(b, way, 1).start()

    def to_pair(b):
        for way in range(2):
            x_copy(b, way, 1).wait_recv()
            at = place(x, way)
            total = xs[way, b, at] + x_near[way, b, at - keep(x, way)] + x_far[way, b, 0]
            for k in range(2):
                for i in range(4):
                    row = pl.multiple_of(b * 128 + k * 64 + (way * 4 + i) * 8, 8)
                    allf[core, pl.ds(row, 8), :] = total[k, :, i * ROOT : (i + 1) * ROOT]
        d_copy(b, core).start()

    lane = lax.broadcasted_iota(jnp.int32, (8, ROOT), 1)
    sub = lax.broadcasted_iota(jnp.int32, (8, ROOT), 0)

    def compute(g):
        for half in range(2):
            first = pl.multiple_of(entry(g, half), 8)
            halo(g, half).wait_recv()
            sums = []
            for i in range(5):
                rows = buf[pl.ds(pl.multiple_of(first + i * HALF_ROWS, 8), HALF_ROWS), :]
                rows = rows.reshape(64, 8, ROOT)
                sums.append(jnp.sum(jnp.sum(rows, axis=0), axis=1, keepdims=True))
            base = half * 32
            for s in range(SEGS):
                mean = (sums[s] + sums[s + 1]) * (1.0 / SEG)
                mean_ref[base + s * 8 : base + s * 8 + 8, :] = jnp.broadcast_to(mean, (8, ROOT))
            absent = (chip == 15, 3) if half == 0 else (chip == 0, 0)
            for ch in range(8):
                first_stage(
                    buf, first, SEGS, ch, tabs, mean_ref, base, mid_ref, high_ref, low_ref, ch * 256
                )
            for c0 in range(0, 8, CHUNK):
                sl = slice(c0 * 256, (c0 + CHUNK) * 256)
                sq = squares(high_ref[sl, :], low_ref[sl, :], tabs[1], tabs[2])
                for ch in range(c0, c0 + CHUNK):
                    power = jnp.zeros((64, ROOT), F32)
                    for s in range(SEGS):
                        r = (ch - c0) * 256 + s * 64
                        sqs = sq[r : r + 64]
                        if s == absent[1]:
                            sqs = jnp.where(absent[0], 0.0, sqs)
                        power = power + sqs
                    at = ch * 128 + 64 * half
                    pow_ref[at : at + 64, :] = power
            sq = squares(*split(mid_ref[base : base + 32, :]), tabs[1], tabs[2])
            middle = jnp.zeros((8, ROOT), F32)
            for s in range(SEGS):
                sqs = sq[s * 8 : s * 8 + 8]
                if s == absent[1]:
                    sqs = jnp.where(absent[0], 0.0, sqs)
                middle = middle + sqs
            zero = pow_ref[pl.ds(64 * half, 8, 128), :]
            last = jnp.sum(jnp.where(lane == ROOT - 1, zero, 0.0), axis=1, keepdims=True)
            spot = lane == 48 * half + 8 * g + sub
            edge_z[0] = jnp.where(spot, jnp.broadcast_to(last, (8, ROOT)), edge_z[0])
            pow_ref[pl.ds(64 * half, 8, 128), :] = jnp.where(lax.rem(lane, 4) >= 2, middle, zero)
        for i in range(8):
            block = pow_ref[i * 128 : (i + 1) * 128, :].T
            lanes = slice((i % 4) * ROOT, (i % 4 + 1) * ROOT)
            for chunk in range(4):
                spot = ((0, 2, 3, 1)[chunk] if i < 4 else chunk) * 32
                zs[i // 4, g, spot : spot + 32, lanes] = block[chunk * 32 : chunk * 32 + 32]

    def pair_arrival(g, half):
        to = entry(g, half) + (2 * other + half) * HALF_ROWS
        return remote(
            x_ref.at[pl.ds(0, 1024), :],
            buf.at[pl.ds(to, 1024), :],
            pair_send.at[g, half],
            pair_recv.at[g, half],
            "tm",
            device(z, x, other),
        )

    for g in range(GROUPS):
        for half in range(2):
            load(g, half).start()
    barrier = pltpu.get_barrier_semaphore()
    peers = [("tm", device(z, x, other))]
    for step in (1, 15):
        peers.append(("tm", lax.rem(chip + step, 16) * 2 + core))
    for step in (1, 2, 3):
        peers.append(("tm", device(lax.rem(z + step, 4), x, core)))
        peers.append(("tm", device(z, lax.rem(x + step, 4), core)))
        peers.append(("chan", lax.rem(y + step, 4)))
    for axis, index in peers:
        pl.semaphore_signal(
            barrier, inc=1, device_id={axis: index}, device_id_type=pl.DeviceIdType.MESH
        )
    pl.semaphore_wait(barrier, len(peers))
    def arrived(g):
        for half in range(2):
            load(g, half).wait()
            pair_arrival(g, half).wait_recv()
            by_relay = (core == 1) & (x == 3 * half)

            @pl.when(by_relay)
            def _():
                hop(g, half).start()

            @pl.when(jnp.logical_not(by_relay))
            def _():
                halo(g, half).start()

    def forward(g):
        @pl.when(relays)
        def _():
            hop(g, 0).wait_recv()
            onward(g).start()

    for g in range(AHEAD + 1):
        for half in range(2):
            pair(g, half).start()
    edge_z[0] = jnp.zeros((8, ROOT), F32)
    for g in range(AHEAD):
        arrived(g)
    forward(0)

    def step(g, carry):
        @pl.when(g < GROUPS - AHEAD - 1)
        def _():
            for half in range(2):
                pair(g + AHEAD + 1, half).start()

        @pl.when(g < GROUPS - AHEAD)
        def _():
            arrived(g + AHEAD)

        @pl.when(g < GROUPS - 1)
        def _():
            forward(g + 1)

        @pl.when(g < GROUPS)
        def _():
            compute(g)
            z_first(g)

        @pl.when(g == GROUPS - 1)
        def _():
            for s in (1, 2, 3):
                edge_copy(0, s).start()

        @pl.when((g >= 1) & (g < GROUPS + 1))
        def _():
            z_second(g - 1)

        @pl.when((g >= 2) & (g < GROUPS + 2))
        def _():
            z_last(g - 2)

        @pl.when((g >= 3) & (g < GROUPS + 2) & (lax.rem(g, 2) == 1))
        def _():
            x_first((g - 3) // 2)

        @pl.when((g >= 4) & (g < GROUPS + 3) & (lax.rem(g, 2) == 0))
        def _():
            x_second((g - 4) // 2)

        @pl.when((g >= 5) & (lax.rem(g, 2) == 1))
        def _():
            to_pair((g - 5) // 2)

        @pl.when(g == GROUPS + 1)
        def _():
            total = edge_z[0]
            for s in (1, 2, 3):
                edge_copy(0, s).wait_recv()
                total = total + edge_z[s]
            edge_x[0] = total
            for s in (1, 2, 3):
                edge_copy(1, s).start()

        @pl.when(g == GROUPS + 3)
        def _():
            total = edge_x[0]
            for s in (1, 2, 3):
                edge_copy(1, s).wait_recv()
                total = total + edge_x[s]
            edge_sum[0] = total
            edge_copy(2, 0).start()

        return carry

    lax.fori_loop(0, GROUPS + 4, step, 0)
    for b in range(BATCHES):
        d_copy(b, other).wait_recv()
    lane_row = lax.broadcasted_iota(jnp.int32, (1, ROOT), 1)
    pieces = []
    for par in range(2):
        stacked = []
        for h in range(2):
            near = allf[h, pl.ds(4 * core + par, 48, 8), :]
            far = allf[h, pl.ds(4 * core + par + 2, 48, 8), :]
            stacked.append(jnp.concatenate([near, far], 1))
        value = jnp.concatenate(stacked, 0)
        high, rest = split(value)
        low = rest.astype(F32)
        rest = (value - high.astype(F32)) - low
        placed = dot(high, perm_ref[...]) + dot(low.astype(BF16), perm_ref[...])
        placed = placed + dot(rest.astype(BF16), perm_ref[...])
        factor = jnp.full((1, ROOT), 2.0 * scale, F32)
        if par == 0:
            factor = jnp.where((lane_row == 0) & (t == 0), scale, factor)
        for kind in range(2):
            out = placed[:, kind * ROOT : (kind + 1) * ROOT] * factor
            for h in range(2):
                at = h * 96 + kind * 48
                power_out[at : at + 48, par * ROOT : (par + 1) * ROOT] = out[h * 48 : h * 48 + 48]
            pieces.append(out)
    sums = []
    for par in range(2):
        both = pieces[2 * par] + pieces[2 * par + 1]
        sums.append(jnp.sum(both, axis=0, keepdims=True))
    mean_buf[0] = jnp.broadcast_to(jnp.concatenate(sums, 1), (8, 256))
    for s in (1, 2, 3):
        mean_copy(s).start()

    def drain(g, carry):
        for way in range(2):
            for step in range(2):
                z_copy(g, way, step).wait_send()
            pair(g, way).wait_send()
            halo(g, way).wait_send()

        @pl.when(relays)
        def _():
            onward(g).wait_send()

        return carry

    lax.fori_loop(0, GROUPS, drain, 0)
    for b in range(BATCHES):
        for way in range(2):
            for step in range(2):
                x_copy(b, way, step).wait_send()
        d_copy(b, core).wait_send()
    for s in (1, 2, 3):
        edge_copy(0, s).wait_send()
        edge_copy(1, s).wait_send()
    edge_copy(2, 0).wait_recv()
    edge_copy(2, 0).wait_send()
    for h in range(2):
        mine = jnp.where(core == h, edge_sum[0], edge_sum[1])
        row = jnp.sum(mine, axis=0, keepdims=True) * scale
        edge_out[:, h * 96 : h * 96 + 96] = row[:, :96]
    mean = mean_buf[0]
    for s in (1, 2, 3):
        mean_copy(s).wait_recv()
        mean = mean + mean_buf[s]
    mean_out[...] = mean[:1] * (1.0 / 768.0)
    for s in (1, 2, 3):
        mean_copy(s).wait_send()


def per_device(strain):
    rows = strain.shape[0]
    tabs_np, energy = tables()
    tabs = [jnp.asarray(t) for t in tabs_np]
    groups = rows // 8
    x4 = strain.reshape(groups, 8, ROOT, ROOT).transpose(0, 2, 1, 3)
    x2 = x4.reshape(groups * 1024, ROOT)
    vmem = pl.BlockSpec(memory_space=pltpu.VMEM)
    dma = pltpu.SemaphoreType.DMA
    power, edge, mean = pl.pallas_call(
        functools.partial(welch_kernel, 1.0 / (63.0 * energy)),
        out_shape=[
            jax.ShapeDtypeStruct((192, 256), F32),
            jax.ShapeDtypeStruct((1, 192), F32),
            jax.ShapeDtypeStruct((1, 256), F32),
        ],
        in_specs=[pl.BlockSpec(memory_space=pl.ANY)] + [vmem] * len(tabs),
        out_specs=[vmem] * 3,
        scratch_shapes=[
            pltpu.VMEM((GROUPS * HALF_ROWS, ROOT), F32),
            dma((GROUPS,)),
            dma((GROUPS,)),
            pltpu.VMEM((GROUPS * 2 * ENTRY_ROWS, ROOT), F32),
            pltpu.VMEM((64, ROOT), F32),
            pltpu.VMEM((64, 256), F32),
            pltpu.VMEM((2048, 256), BF16),
            pltpu.VMEM((2048, 256), BF16),
            pltpu.VMEM((1024, ROOT), F32),
            pltpu.VMEM((2, GROUPS, 128, 512), F32),
            pltpu.VMEM((2, GROUPS, 64, 512), F32),
            pltpu.VMEM((2, GROUPS, 32, 512), F32),
            pltpu.VMEM((2, BATCHES, 4, 2, 8, 512), F32),
            pltpu.VMEM((2, BATCHES, 2, 2, 8, 512), F32),
            pltpu.VMEM((2, BATCHES, 1, 2, 8, 512), F32),
            pltpu.VMEM((2, GROUPS * 64, ROOT), F32),
            pltpu.VMEM((4, 8, ROOT), F32),
            pltpu.VMEM((4, 8, ROOT), F32),
            pltpu.VMEM((2, 8, ROOT), F32),
            pltpu.VMEM((4, 8, 256), F32),
            dma((GROUPS, 2)),
            dma((GROUPS, 2)),
            dma((GROUPS, 2)),
            dma((GROUPS, 2)),
            dma((GROUPS, 2)),
            dma((2, GROUPS, 2)),
            dma((2, GROUPS, 2)),
            dma((2, BATCHES, 2)),
            dma((2, BATCHES, 2)),
            dma((BATCHES,)),
            dma((BATCHES,)),
            dma((3, 4)),
            dma((3, 4)),
            dma((4,)),
            dma((4,)),
        ],
        compiler_params=pltpu.CompilerParams(
            collective_id=0, has_side_effects=True, vmem_limit_bytes=60 * 1024 * 1024
        ),
    )(x2, *tabs)
    nyquist = edge.reshape(rows)
    return power, nyquist, mean.reshape(256)


def solution(mesh):
    return jax.shard_map(
        per_device,
        mesh=mesh,
        in_specs=(P("chan", "tm"),),
        out_specs=(P("chan", "tm"), P("chan"), P("tm")),
        check_vma=False,
    )
```

```python
import functools

import jax
import jax.numpy as jnp
import numpy as np
from jax import lax
from jax.experimental import pallas as pl
from jax.experimental.pallas import tpu as pltpu
from jax.sharding import PartitionSpec as P

SEG = 16384
ROOT = 128
F32 = jnp.float32
BF16 = jnp.bfloat16
STRIDE = 8
CHUNK = 4


def split(values):
    high = values.astype(BF16)
    low = (values - high.astype(F32)).astype(BF16)
    return high, low


def split_np(values):
    high = values.astype(np.float32).astype(BF16)
    low = (values - high.astype(np.float64)).astype(np.float32).astype(BF16)
    return high, low


def lane_bins():
    lane = np.arange(ROOT)
    owner, part = lane // 4, lane % 4
    return np.where(part < 2, 2 * owner + part, 127 - 2 * owner - (part - 2))


def tables():
    turn = 2.0 * np.pi / ROOT
    a = np.arange(ROOT)
    k1 = np.arange(64)
    cos_rows = np.cos(turn * ((k1[:, None] * a) % ROOT))
    sin_rows = -np.sin(turn * ((k1[:, None] * a) % ROOT))
    sin_rows[0] = 1.0 - 2.0 * (a % 2)
    first = np.concatenate([cos_rows, sin_rows], 0)
    first_high, first_low = split_np(first)
    first_high = np.concatenate([first_high, first_high], 1)
    first_low = np.concatenate([first_low, first_low], 1)
    q = lane_bins()
    cos_q = np.cos(turn * ((a[:, None] * q) % ROOT))
    sin_q = np.sin(turn * ((a[:, None] * q) % ROOT))
    last = np.concatenate(
        [np.concatenate([cos_q, -sin_q], 1), np.concatenate([sin_q, cos_q], 1)], 0
    )
    last_high, last_low = split_np(last)
    long_turn = 2.0 * np.pi / SEG
    twist = long_turn * (k1[:, None] * a)
    cos_twist = np.cos(twist).astype(np.float32)
    sin_twist = np.sin(twist).astype(np.float32)
    mid = long_turn * 64 * a
    mid_twist = np.stack([np.cos(mid), np.sin(mid)] + [0 * mid] * 6).astype(np.float32)
    n = np.arange(SEG, dtype=np.float64)
    window = (0.5 - 0.5 * np.cos(2.0 * np.pi * n / SEG)).astype(np.float32)
    slot, kind, k = np.meshgrid(np.arange(2), np.arange(2), np.arange(64), indexing="ij")
    place = np.where(slot == 0, k, np.where(k == 0, 64, 128 - k)) + 128 * kind
    perm = np.zeros((256, 256), np.float32)
    perm[np.arange(256), place.reshape(-1)] = 1.0
    energy = float(np.sum(window.astype(np.float64) ** 2))
    return (
        [
            np.concatenate([first_high, first_low], 0),
            last_high,
            last_low,
            cos_twist,
            sin_twist,
            mid_twist,
            window.reshape(ROOT, ROOT),
            perm.astype(BF16),
        ],
        energy,
    )


def dot(a, b):
    return jnp.dot(a, b, preferred_element_type=F32)


def first_stage(blocks, start, pair, ch, tabs, mean_ref, mean_base, mid_ref, mid_row, high_ref, low_ref):
    t_ref, vh_ref, vl_ref, c_ref, s_ref, mid_tw, w_ref = tabs
    w0, w1 = w_ref[:64, :], w_ref[64:, :]
    row = lax.broadcasted_iota(jnp.int32, (8, 256), 0)
    highs, lows = [], []
    for s in (2 * pair, 2 * pair + 1):
        mean = mean_ref[pl.ds(mean_base + s * 8 + ch, 1), :]
        r0, b0, b1 = blocks, start + s * 512, start + s * 512 + 512
        x0 = (r0[pl.ds(b0 + ch, 64, STRIDE), :] - mean) * w0
        x1 = (r0[pl.ds(b1 + ch, 64, STRIDE), :] - mean) * w1
        high, low = split(jnp.concatenate([x0, x1], 0))
        highs.append(high)
        lows.append(low)
    x = jnp.concatenate(
        [jnp.concatenate(highs, 1), jnp.concatenate(lows, 1)], 0
    )
    both = dot(t_ref[...], x)
    d = both[:128] + both[128:]
    fr = d[:64]
    fi = jnp.concatenate([jnp.where(row == 0, 0.0, d[64:72]), d[72:]], 0)
    mid = d[64:65]
    c, s_ = c_ref[...], s_ref[...]
    for i in range(2):
        s = 2 * pair + i
        lanes = slice(i * ROOT, (i + 1) * ROOT)
        tr = fr[:, lanes] * c + fi[:, lanes] * s_
        ti = fi[:, lanes] * c - fr[:, lanes] * s_
        put = ch * 128 + 64 * i
        high, low = split(jnp.concatenate([tr, ti], 1))
        high_ref[pl.ds(put, 64), :] = high
        low_ref[pl.ds(put, 64), :] = low
        m = mid[:, lanes]
        mid_ref[pl.ds(mid_row + s * 8 + ch, 1), :] = jnp.concatenate(
            [m * mid_tw[0:1, :], -m * mid_tw[1:2, :]], 1
        )


def squares(high, low, vh_ref, vl_ref):
    o = dot(high, vh_ref[...]) + dot(low, vh_ref[...]) + dot(high, vl_ref[...])
    return o[:, :ROOT] * o[:, :ROOT] + o[:, ROOT:] * o[:, ROOT:]


GROUPS = 6
HALF_ROWS = 512
ENTRY_ROWS = 5 * HALF_ROWS
SEGS = 4
BATCHES = 3
AHEAD = 2


def remote(src, dst, send, recv, axis, index, **more):
    return pltpu.make_async_remote_copy(
        src_ref=src,
        dst_ref=dst,
        send_sem=send,
        recv_sem=recv,
        device_id={axis: index, **more},
        device_id_type=pl.DeviceIdType.MESH,
    )


def twin(r):
    return r + 1 - 2 * lax.rem(r, 2)


def partners(r, way):
    if way == 0:
        return twin(r), 3 - r
    return 3 - r, twin(r)


def place(r, way):
    if way == 0:
        return lax.rem(2 * r - r // 2, 4)
    return r


def keep(r, way):
    return place(r, way) // 2 * 2


def welch_kernel(scale, x_ref, *refs):
    tabs, perm_ref, refs = refs[:7], refs[7], refs[8:]
    power_out, edge_out, mean_out = refs[:3]
    (relay, relay_send, relay_recv), refs = refs[3:6], refs[:3] + refs[6:]
    (buf, mean_ref, mid_ref, high_ref, low_ref, pow_ref) = refs[3:9]
    (zs, z_near, z_far, xs, x_near, x_far, allf) = refs[9:16]
    (edge_z, edge_x, edge_sum, mean_buf, mean_sum), refs = refs[16:21], refs[:20] + refs[21:]
    (load_sem, pair_send, pair_recv, halo_send, halo_recv, z_send, z_recv) = refs[20:27]
    (x_send, x_recv, d_send, d_recv, e_send, e_recv, m_send, m_recv) = refs[27:]
    y = lax.axis_index("chan")
    t = lax.axis_index("tm")
    core = lax.rem(t, 2)
    chip = t // 2
    x = lax.rem(chip, 4)
    z = chip // 4
    other = 1 - core
    device = lambda zz, xx, cc: (zz * 4 + xx) * 2 + cc

    def entry(g, half):
        return (g * 2 + half) * ENTRY_ROWS

    def load(g, half):
        row = (12 * core + 6 * half + g) * 1024
        to = entry(g, half) + (2 * core + half) * HALF_ROWS
        return pltpu.make_async_copy(
            x_ref.at[pl.ds(row, 1024), :], buf.at[pl.ds(to, 1024), :], load_sem.at[g, half]
        )

    def pair(g, half):
        row = (12 * other + 6 * half + g) * 1024
        to = entry(g, half) + (2 * core + half) * HALF_ROWS
        return remote(
            x_ref.at[pl.ds(row, 1024), :],
            buf.at[pl.ds(to, 1024), :],
            pair_send.at[g, half],
            pair_recv.at[g, half],
            "tm",
            device(z, x, other),
        )

    def halo(g, half):
        there = entry(g, half) + (1 - half) * 4 * HALF_ROWS
        here = entry(g, half) + half * 4 * HALF_ROWS
        target = lax.rem(chip + (15 if half == 0 else 1), 16)
        return remote(
            buf.at[pl.ds(here, HALF_ROWS), :],
            buf.at[pl.ds(there, HALF_ROWS), :],
            halo_send.at[g, half],
            halo_recv.at[g, half],
            "tm",
            target * 2 + core,
        )

    def hop(g, half, to):
        here = entry(g, half) + half * 4 * HALF_ROWS
        return remote(
            buf.at[pl.ds(here, HALF_ROWS), :],
            relay.at[pl.ds(g * HALF_ROWS, HALF_ROWS), :],
            halo_send.at[g, half],
            relay_recv.at[g],
            "tm",
            to,
        )

    def onward(g, half, to):
        there = entry(g, half) + (1 - half) * 4 * HALF_ROWS
        return remote(
            relay.at[pl.ds(g * HALF_ROWS, HALF_ROWS), :],
            buf.at[pl.ds(there, HALF_ROWS), :],
            relay_send.at[g],
            halo_recv.at[g, half],
            "tm",
            to,
        )

    relays = (core == 1) & ((x == 0) | (x == 3))
    relay_half = x // 3
    relay_to = device(z, 3 - x, core)

    def z_copy(g, way, step):
        near, far = partners(z, way)
        if step == 0:
            start, rows, into, to = (2 - keep(z, way)) * 32, 64, z_near, near
        else:
            start, rows, into, to = place(far, way) * 32, 32, z_far, far
        return remote(
            zs.at[way, g, pl.ds(start, rows), :],
            into.at[way, g],
            z_send.at[way, g, step],
            z_recv.at[way, g, step],
            "tm",
            device(to, x, core),
        )

    def x_copy(b, way, step):
        near, far = partners(x, way)
        if step == 0:
            start, size, into, to = 2 - keep(x, way), 2, x_near, near
        else:
            start, size, into, to = place(far, way), 1, x_far, far
        return remote(
            xs.at[way, b, pl.ds(start, size)],
            into.at[way, b],
            x_send.at[way, b, step],
            x_recv.at[way, b, step],
            "tm",
            device(z, to, core),
        )

    def d_copy(b, half_owner):
        rows = allf.at[half_owner, pl.ds(b * 128, 128), :]
        return remote(rows, rows, d_send.at[b], d_recv.at[b], "tm", device(z, x, other))

    def edge_copy(stage, step):
        if stage == 0:
            return remote(
                edge_z.at[0], edge_z.at[step], e_send.at[0, step], e_recv.at[0, step],
                "tm", device(lax.rem(z + step, 4), x, core),
            )
        if stage == 1:
            return remote(
                edge_x.at[0], edge_x.at[step], e_send.at[1, step], e_recv.at[1, step],
                "tm", device(z, lax.rem(x + step, 4), core),
            )
        return remote(
            edge_sum.at[0], edge_sum.at[1], e_send.at[2, 0], e_recv.at[2, 0],
            "tm", device(z, x, other),
        )

    def mean_copy(step):
        target = core if step % 2 == 0 else other
        return remote(
            mean_buf.at[0], mean_buf.at[step], m_send.at[step], m_recv.at[step],
            "tm", device(z, x, target), chan=lax.rem(y + step // 2, 4),
        )

    def z_first(g):
        for way in range(2):
            z_copy(g, way, 0).start()

    def z_second(g):
        for way in range(2):
            far = partners(z, way)[1]
            z_copy(g, way, 0).wait_recv()
            at = place(far, way)
            rows = pl.ds(pl.multiple_of(at * 32, 32), 32)
            got = pl.ds(pl.multiple_of((at - keep(z, way)) * 32, 32), 32)
            zs[way, g, rows, :] = zs[way, g, rows, :] + z_near[way, g, got, :]
            z_copy(g, way, 1).start()

    def z_last(g):
        for way in range(2):
            z_copy(g, way, 1).wait_recv()
            at = place(z, way)
            rows = pl.ds(pl.multiple_of(at * 32, 32), 32)
            got = pl.ds(pl.multiple_of((at - keep(z, way)) * 32, 32), 32)
            total = zs[way, g, rows, :] + z_near[way, g, got, :] + z_far[way, g]
            for chunk in range(4):
                spot = (0, 2, 3, 1)[chunk] if way == 0 else chunk
                xs[way, g // 2, spot, lax.rem(g, 2)] = total[chunk * 8 : chunk * 8 + 8, :]

    def x_first(b):
        for way in range(2):
            x_copy(b, way, 0).start()

    def x_second(b):
        for way in range(2):
            far = partners(x, way)[1]
            x_copy(b, way, 0).wait_recv()
            at = place(far, way)
            xs[way, b, at] = xs[way, b, at] + x_near[way, b, at - keep(x, way)]
            x_copy(b, way, 1).start()

    def to_pair(b):
        for way in range(2):
            x_copy(b, way, 1).wait_recv()
            at = place(x, way)
            total = xs[way, b, at] + x_near[way, b, at - keep(x, way)] + x_far[way, b, 0]
            both = total[0] + total[1]
            column = both[:, :ROOT] + both[:, ROOT : 2 * ROOT]
            column = column + (both[:, 2 * ROOT : 3 * ROOT] + both[:, 3 * ROOT :])
            mean_buf[0] = mean_buf[0] + column
            for k in range(2):
                for i in range(4):
                    row = pl.multiple_of(b * 128 + k * 64 + (way * 4 + i) * 8, 8)
                    allf[core, pl.ds(row, 8), :] = total[k, :, i * ROOT : (i + 1) * ROOT]
        d_copy(b, core).start()

        @pl.when(b == BATCHES - 1)
        def _():
            for s in range(1, 8):
                mean_copy(s).start()

    lane = lax.broadcasted_iota(jnp.int32, (8, ROOT), 1)
    sub = lax.broadcasted_iota(jnp.int32, (8, ROOT), 0)

    def phase(g, late):
        for half in range(2):
            pair_index = (1 - half) if late else half
            first = pl.multiple_of(entry(g, half), 8)
            if late:
                halo(g, half).wait_recv()
            sums = []
            for i in range(2 * pair_index, 2 * pair_index + 3):
                rows = buf[pl.ds(pl.multiple_of(first + i * HALF_ROWS, 8), HALF_ROWS), :]
                rows = rows.reshape(64, 8, ROOT)
                sums.append(jnp.sum(jnp.sum(rows, axis=0), axis=1, keepdims=True))
            base = half * 32
            for i in range(2):
                mean = (sums[i] + sums[i + 1]) * (1.0 / SEG)
                at = base + (2 * pair_index + i) * 8
                mean_ref[at : at + 8, :] = jnp.broadcast_to(mean, (8, ROOT))
            mid_row = pl.multiple_of(g * 64 + base, 8)
            for ch in range(8):
                first_stage(
                    buf, first, pair_index, ch, tabs, mean_ref, base, mid_ref, mid_row, high_ref, low_ref
                )
            gone = (chip == 15) if half == 0 else (chip == 0)
            for c0 in range(0, 8, CHUNK):
                sl = slice(c0 * 128, (c0 + CHUNK) * 128)
                sq = squares(high_ref[sl, :], low_ref[sl, :], tabs[1], tabs[2])
                for ch in range(c0, c0 + CHUNK):
                    r = (ch - c0) * 128
                    one, two = sq[r : r + 64], sq[r + 64 : r + 128]
                    at = pl.multiple_of(g * 1024 + ch * 128 + 64 * half, 64)
                    if late:
                        if half == 0:
                            two = jnp.where(gone, 0.0, two)
                        else:
                            one = jnp.where(gone, 0.0, one)
                        pow_ref[pl.ds(at, 64), :] = pow_ref[pl.ds(at, 64), :] + (one + two)
                    else:
                        pow_ref[pl.ds(at, 64), :] = one + two
            if not late:
                continue
            sq = squares(*split(mid_ref[pl.ds(mid_row, 32), :]), tabs[1], tabs[2])
            middle = jnp.zeros((8, ROOT), F32)
            for s in range(SEGS):
                sqs = sq[s * 8 : s * 8 + 8]
                if s == 3 * (1 - half):
                    sqs = jnp.where(gone, 0.0, sqs)
                middle = middle + sqs
            zeros = pl.ds(g * 1024 + 64 * half, 8, 128)
            zero = pow_ref[zeros, :]
            last = jnp.sum(jnp.where(lane == ROOT - 1, zero, 0.0), axis=1, keepdims=True)
            spot = lane == 48 * half + 8 * g + sub
            edge_z[0] = jnp.where(spot, jnp.broadcast_to(last, (8, ROOT)), edge_z[0])
            pow_ref[zeros, :] = jnp.where(lax.rem(lane, 4) >= 2, middle, zero)
        if not late:
            return
        for i in range(8):
            block = pow_ref[pl.ds(pl.multiple_of(g * 1024 + i * 128, 128), 128), :].T
            lanes = slice((i % 4) * ROOT, (i % 4 + 1) * ROOT)
            for chunk in range(4):
                spot = ((0, 2, 3, 1)[chunk] if i < 4 else chunk) * 32
                zs[i // 4, g, spot : spot + 32, lanes] = block[chunk * 32 : chunk * 32 + 32]

    def pair_arrival(g, half):
        to = entry(g, half) + (2 * other + half) * HALF_ROWS
        return remote(
            x_ref.at[pl.ds(0, 1024), :],
            buf.at[pl.ds(to, 1024), :],
            pair_send.at[g, half],
            pair_recv.at[g, half],
            "tm",
            device(z, x, other),
        )

    for g in range(GROUPS):
        for half in range(2):
            load(g, half).start()
    barrier = pltpu.get_barrier_semaphore()
    peers = [("tm", device(z, x, other))]
    for step in (1, 15):
        peers.append(("tm", lax.rem(chip + step, 16) * 2 + core))
    for step in (1, 3):
        peers.append(("tm", device(lax.rem(z + step, 4), x, core)))
        peers.append(("tm", device(z, lax.rem(x + step, 4), core)))
    peers.append(("tm", device(lax.rem(z + 2, 4), x, core)))
    peers.append(("tm", device(z, lax.rem(x + 2, 4), core)))
    signals = [{axis: index} for axis, index in peers]
    for step in (1, 2, 3):
        for to in (core, other):
            signals.append({"chan": lax.rem(y + step, 4), "tm": device(z, x, to)})
    for to in signals:
        pl.semaphore_signal(
            barrier, inc=1, device_id=to, device_id_type=pl.DeviceIdType.MESH
        )
    pl.semaphore_wait(barrier, len(signals))
    def arrived(g):
        for half in range(2):
            load(g, half).wait()
            pair_arrival(g, half).wait_recv()
            by_relay = (core == 1) & (x == 3 * half)
            to = device(lax.rem(z + 3 + 2 * half, 4), x, core)

            @pl.when(by_relay)
            def _():
                hop(g, half, to).start()

            @pl.when(jnp.logical_not(by_relay))
            def _():
                halo(g, half).start()

    def forward(g):
        @pl.when(relays)
        def _():
            hop(g, 0, relay_to).wait_recv()
            onward(g, relay_half, relay_to).start()

    for g in range(AHEAD + 1):
        for half in range(2):
            pair(g, half).start()
    edge_z[0] = jnp.zeros((8, ROOT), F32)
    mean_buf[0] = jnp.zeros((8, ROOT), F32)
    for g in range(AHEAD):
        arrived(g)
    phase(0, False)
    forward(0)
    phase(1, False)

    def step(g, carry):
        @pl.when(g < GROUPS - AHEAD - 1)
        def _():
            for half in range(2):
                pair(g + AHEAD + 1, half).start()

        @pl.when(g < GROUPS - AHEAD)
        def _():
            arrived(g + AHEAD)

        @pl.when(g < GROUPS - 1)
        def _():
            forward(g + 1)

        @pl.when(g < GROUPS - 2)
        def _():
            phase(g + 2, False)

        @pl.when(g < GROUPS)
        def _():
            phase(g, True)
            z_first(g)

        @pl.when(g == GROUPS - 1)
        def _():
            for s in (1, 2, 3):
                edge_copy(0, s).start()

        @pl.when((g >= 1) & (g < GROUPS + 1))
        def _():
            z_second(g - 1)

        @pl.when((g >= 2) & (g < GROUPS + 2))
        def _():
            z_last(g - 2)

        @pl.when((g >= 3) & (g < GROUPS + 2) & (lax.rem(g, 2) == 1))
        def _():
            x_first((g - 3) // 2)

        @pl.when((g >= 4) & (g < GROUPS + 3) & (lax.rem(g, 2) == 0))
        def _():
            x_second((g - 4) // 2)

        @pl.when((g >= 5) & (lax.rem(g, 2) == 1))
        def _():
            to_pair((g - 5) // 2)

        @pl.when(g == GROUPS + 1)
        def _():
            total = edge_z[0]
            for s in (1, 2, 3):
                edge_copy(0, s).wait_recv()
                total = total + edge_z[s]
            edge_x[0] = total
            for s in (1, 2, 3):
                edge_copy(1, s).start()

        @pl.when(g == GROUPS + 3)
        def _():
            total = edge_x[0]
            for s in (1, 2, 3):
                edge_copy(1, s).wait_recv()
                total = total + edge_x[s]
            edge_sum[0] = total
            edge_copy(2, 0).start()

        return carry

    lax.fori_loop(0, GROUPS + 4, step, 0)
    for b in range(BATCHES):
        d_copy(b, other).wait_recv()
    total = mean_buf[0]
    for s in range(1, 8):
        mean_copy(s).wait_recv()
        total = total + mean_buf[s]
    mean_sum[...] = total
    lane_row = lax.broadcasted_iota(jnp.int32, (1, ROOT), 1)
    for par in range(2):
        stacked = []
        for h in range(2):
            near = allf[h, pl.ds(4 * core + par, 48, 8), :]
            far = allf[h, pl.ds(4 * core + par + 2, 48, 8), :]
            stacked.append(jnp.concatenate([near, far], 1))
        row = jnp.concatenate(
            [mean_sum[pl.ds(4 * core + par, 1), :], mean_sum[pl.ds(4 * core + par + 2, 1), :]], 1
        )
        value = jnp.concatenate(stacked + [jnp.broadcast_to(row, (8, 256))], 0)
        high, rest = split(value)
        low = rest.astype(F32)
        rest = (value - high.astype(F32)) - low
        placed = dot(high, perm_ref[...]) + dot(low.astype(BF16), perm_ref[...])
        placed = placed + dot(rest.astype(BF16), perm_ref[...])
        factor = jnp.full((1, ROOT), 2.0 * scale, F32)
        if par == 0:
            factor = jnp.where((lane_row == 0) & (t == 0), scale, factor)
        for kind in range(2):
            out = placed[:, kind * ROOT : (kind + 1) * ROOT] * factor
            for h in range(2):
                at = h * 96 + kind * 48
                power_out[at : at + 48, par * ROOT : (par + 1) * ROOT] = out[h * 48 : h * 48 + 48]
        row = (placed[96:97, :ROOT] + placed[96:97, ROOT:]) * factor
        mean_out[:, par * ROOT : (par + 1) * ROOT] = row * (1.0 / 768.0)

    def drain(g, carry):
        for way in range(2):
            for step in range(2):
                z_copy(g, way, step).wait_send()
            pair(g, way).wait_send()
            halo(g, way).wait_send()

        @pl.when(relays)
        def _():
            onward(g, relay_half, relay_to).wait_send()

        return carry

    lax.fori_loop(0, GROUPS, drain, 0)
    for b in range(BATCHES):
        for way in range(2):
            for step in range(2):
                x_copy(b, way, step).wait_send()
        d_copy(b, core).wait_send()
    for s in (1, 2, 3):
        edge_copy(0, s).wait_send()
        edge_copy(1, s).wait_send()
    edge_copy(2, 0).wait_recv()
    edge_copy(2, 0).wait_send()
    for h in range(2):
        mine = jnp.where(core == h, edge_sum[0], edge_sum[1])
        row = jnp.sum(mine, axis=0, keepdims=True) * scale
        edge_out[:, h * 96 : h * 96 + 96] = row[:, :96]
    for s in range(1, 8):
        mean_copy(s).wait_send()


def per_device(strain):
    rows = strain.shape[0]
    tabs_np, energy = tables()
    tabs = [jnp.asarray(t) for t in tabs_np]
    groups = rows // 8
    x4 = strain.reshape(groups, 8, ROOT, ROOT).transpose(0, 2, 1, 3)
    x2 = x4.reshape(groups * 1024, ROOT)
    vmem = pl.BlockSpec(memory_space=pltpu.VMEM)
    dma = pltpu.SemaphoreType.DMA
    power, edge, mean = pl.pallas_call(
        functools.partial(welch_kernel, 1.0 / (63.0 * energy)),
        out_shape=[
            jax.ShapeDtypeStruct((192, 256), F32),
            jax.ShapeDtypeStruct((1, 192), F32),
            jax.ShapeDtypeStruct((1, 256), F32),
        ],
        in_specs=[pl.BlockSpec(memory_space=pl.ANY)] + [vmem] * len(tabs),
        out_specs=[vmem] * 3,
        scratch_shapes=[
            pltpu.VMEM((GROUPS * HALF_ROWS, ROOT), F32),
            dma((GROUPS,)),
            dma((GROUPS,)),
            pltpu.VMEM((GROUPS * 2 * ENTRY_ROWS, ROOT), F32),
            pltpu.VMEM((64, ROOT), F32),
            pltpu.VMEM((GROUPS * 64, 256), F32),
            pltpu.VMEM((1024, 256), BF16),
            pltpu.VMEM((1024, 256), BF16),
            pltpu.VMEM((GROUPS * 1024, ROOT), F32),
            pltpu.VMEM((2, GROUPS, 128, 512), F32),
            pltpu.VMEM((2, GROUPS, 64, 512), F32),
            pltpu.VMEM((2, GROUPS, 32, 512), F32),
            pltpu.VMEM((2, BATCHES, 4, 2, 8, 512), F32),
            pltpu.VMEM((2, BATCHES, 2, 2, 8, 512), F32),
            pltpu.VMEM((2, BATCHES, 1, 2, 8, 512), F32),
            pltpu.VMEM((2, GROUPS * 64, ROOT), F32),
            pltpu.VMEM((4, 8, ROOT), F32),
            pltpu.VMEM((4, 8, ROOT), F32),
            pltpu.VMEM((2, 8, ROOT), F32),
            pltpu.VMEM((8, 8, ROOT), F32),
            pltpu.VMEM((8, ROOT), F32),
            dma((GROUPS, 2)),
            dma((GROUPS, 2)),
            dma((GROUPS, 2)),
            dma((GROUPS, 2)),
            dma((GROUPS, 2)),
            dma((2, GROUPS, 2)),
            dma((2, GROUPS, 2)),
            dma((2, BATCHES, 2)),
            dma((2, BATCHES, 2)),
            dma((BATCHES,)),
            dma((BATCHES,)),
            dma((3, 4)),
            dma((3, 4)),
            dma((8,)),
            dma((8,)),
        ],
        compiler_params=pltpu.CompilerParams(
            collective_id=0, has_side_effects=True, vmem_limit_bytes=60 * 1024 * 1024
        ),
    )(x2, *tabs)
    nyquist = edge.reshape(rows)
    return power, nyquist, mean.reshape(256)


def solution(mesh):
    return jax.shard_map(
        per_device,
        mesh=mesh,
        in_specs=(P("chan", "tm"),),
        out_specs=(P("chan", "tm"), P("chan"), P("tm")),
        check_vma=False,
    )
```

```python
import functools

import jax
import jax.numpy as jnp
import numpy as np
from jax import lax
from jax.experimental import pallas as pl
from jax.experimental.pallas import tpu as pltpu
from jax.sharding import PartitionSpec as P

SEG = 16384
ROOT = 128
F32 = jnp.float32
BF16 = jnp.bfloat16
STRIDE = 8
CHUNK = 4


def split(values):
    high = values.astype(BF16)
    low = (values - high.astype(F32)).astype(BF16)
    return high, low


def split_np(values):
    high = values.astype(np.float32).astype(BF16)
    low = (values - high.astype(np.float64)).astype(np.float32).astype(BF16)
    return high, low


def lane_bins():
    lane = np.arange(ROOT)
    owner, part = lane // 4, lane % 4
    return np.where(part < 2, 2 * owner + part, 127 - 2 * owner - (part - 2))


def tables():
    turn = 2.0 * np.pi / ROOT
    a = np.arange(ROOT)
    k1 = np.arange(64)
    cos_rows = np.cos(turn * ((k1[:, None] * a) % ROOT))
    sin_rows = -np.sin(turn * ((k1[:, None] * a) % ROOT))
    sin_rows[0] = 1.0 - 2.0 * (a % 2)
    first = np.concatenate([cos_rows, sin_rows], 0)
    first_high, first_low = split_np(first)
    first_high = np.concatenate([first_high, first_high], 1)
    first_low = np.concatenate([first_low, first_low], 1)
    q = lane_bins()
    cos_q = np.cos(turn * ((a[:, None] * q) % ROOT))
    sin_q = np.sin(turn * ((a[:, None] * q) % ROOT))
    last = np.concatenate(
        [np.concatenate([cos_q, -sin_q], 1), np.concatenate([sin_q, cos_q], 1)], 0
    )
    last_high, last_low = split_np(last)
    long_turn = 2.0 * np.pi / SEG
    twist = long_turn * (k1[:, None] * a)
    cos_twist = np.cos(twist).astype(np.float32)
    sin_twist = np.sin(twist).astype(np.float32)
    mid = long_turn * 64 * a
    mid_twist = np.stack([np.cos(mid), np.sin(mid)] + [0 * mid] * 6).astype(np.float32)
    n = np.arange(SEG, dtype=np.float64)
    window = (0.5 - 0.5 * np.cos(2.0 * np.pi * n / SEG)).astype(np.float32)
    slot, kind, k = np.meshgrid(np.arange(2), np.arange(2), np.arange(64), indexing="ij")
    place = np.where(slot == 0, k, np.where(k == 0, 64, 128 - k)) + 128 * kind
    perm = np.zeros((256, 256), np.float32)
    perm[np.arange(256), place.reshape(-1)] = 1.0
    energy = float(np.sum(window.astype(np.float64) ** 2))
    return (
        [
            np.concatenate([first_high, first_low], 0),
            last_high,
            last_low,
            cos_twist,
            sin_twist,
            mid_twist,
            window.reshape(ROOT, ROOT),
            perm.astype(BF16),
        ],
        energy,
    )


def dot(a, b):
    return jnp.dot(a, b, preferred_element_type=F32)


def first_stage(blocks, start, pair, ch, tabs, mean_ref, mean_base, mid_ref, mid_row, high_ref, low_ref):
    t_ref, vh_ref, vl_ref, c_ref, s_ref, mid_tw, w_ref = tabs
    w0, w1 = w_ref[:64, :], w_ref[64:, :]
    row = lax.broadcasted_iota(jnp.int32, (8, 256), 0)
    highs, lows = [], []
    for s in (2 * pair, 2 * pair + 1):
        mean = mean_ref[pl.ds(mean_base + s * 8 + ch, 1), :]
        r0, b0, b1 = blocks, start + s * 512, start + s * 512 + 512
        x0 = (r0[pl.ds(b0 + ch, 64, STRIDE), :] - mean) * w0
        x1 = (r0[pl.ds(b1 + ch, 64, STRIDE), :] - mean) * w1
        high, low = split(jnp.concatenate([x0, x1], 0))
        highs.append(high)
        lows.append(low)
    x = jnp.concatenate(
        [jnp.concatenate(highs, 1), jnp.concatenate(lows, 1)], 0
    )
    both = dot(t_ref[...], x)
    d = both[:128] + both[128:]
    fr = d[:64]
    fi = jnp.concatenate([jnp.where(row == 0, 0.0, d[64:72]), d[72:]], 0)
    mid = d[64:65]
    c, s_ = c_ref[...], s_ref[...]
    for i in range(2):
        s = 2 * pair + i
        lanes = slice(i * ROOT, (i + 1) * ROOT)
        tr = fr[:, lanes] * c + fi[:, lanes] * s_
        ti = fi[:, lanes] * c - fr[:, lanes] * s_
        put = ch * 128 + 64 * i
        high, low = split(jnp.concatenate([tr, ti], 1))
        high_ref[pl.ds(put, 64), :] = high
        low_ref[pl.ds(put, 64), :] = low
        m = mid[:, lanes]
        mid_ref[pl.ds(mid_row + s * 8 + ch, 1), :] = jnp.concatenate(
            [m * mid_tw[0:1, :], -m * mid_tw[1:2, :]], 1
        )


def squares(high, low, vh_ref, vl_ref):
    o = dot(high, vh_ref[...]) + dot(low, vh_ref[...]) + dot(high, vl_ref[...])
    return o[:, :ROOT] * o[:, :ROOT] + o[:, ROOT:] * o[:, ROOT:]


GROUPS = 6
HALF_ROWS = 512
ENTRY_ROWS = 5 * HALF_ROWS
SEGS = 4
ENTRIES = 2 * GROUPS
BATCHES = GROUPS
AHEAD = 2


def remote(src, dst, send, recv, axis, index, **more):
    return pltpu.make_async_remote_copy(
        src_ref=src,
        dst_ref=dst,
        send_sem=send,
        recv_sem=recv,
        device_id={axis: index, **more},
        device_id_type=pl.DeviceIdType.MESH,
    )


def twin(r):
    return r + 1 - 2 * lax.rem(r, 2)


def partners(r, way):
    if way == 0:
        return twin(r), 3 - r
    return 3 - r, twin(r)


def place(r, way):
    if way == 0:
        return lax.rem(2 * r - r // 2, 4)
    return r


def keep(r, way):
    return place(r, way) // 2 * 2


def welch_kernel(scale, x_ref, *refs):
    tabs, perm_ref, refs = refs[:7], refs[7], refs[8:]
    power_out, edge_out, mean_out = refs[:3]
    (relay, relay_send, relay_recv, spread), refs = refs[3:7], refs[:3] + refs[7:]
    (buf, mean_ref, mid_ref, high_ref, low_ref, pow_ref) = refs[3:9]
    (zs, z_near, z_far, xs, x_near, x_far, allf) = refs[9:16]
    (edge_z, edge_x, edge_sum, mean_buf, mean_sum), refs = refs[16:21], refs[:20] + refs[21:]
    (load_sem, pair_send, pair_recv, halo_send, halo_recv, z_send, z_recv) = refs[20:27]
    (x_send, x_recv, d_send, d_recv, e_send, e_recv, m_send, m_recv) = refs[27:]
    y = lax.axis_index("chan")
    t = lax.axis_index("tm")
    core = lax.rem(t, 2)
    chip = t // 2
    x = lax.rem(chip, 4)
    z = chip // 4
    other = 1 - core
    device = lambda zz, xx, cc: (zz * 4 + xx) * 2 + cc

    def entry(g, half):
        return (g * 2 + half) * ENTRY_ROWS

    def load(g, half):
        row = (12 * core + 6 * half + g) * 1024
        to = entry(g, half) + (2 * core + half) * HALF_ROWS
        return pltpu.make_async_copy(
            x_ref.at[pl.ds(row, 1024), :], buf.at[pl.ds(to, 1024), :], load_sem.at[g, half]
        )

    def pair(g, half):
        row = (12 * other + 6 * half + g) * 1024
        to = entry(g, half) + (2 * core + half) * HALF_ROWS
        return remote(
            x_ref.at[pl.ds(row, 1024), :],
            buf.at[pl.ds(to, 1024), :],
            pair_send.at[g, half],
            pair_recv.at[g, half],
            "tm",
            device(z, x, other),
        )

    def halo(g, half):
        there = entry(g, half) + (1 - half) * 4 * HALF_ROWS
        here = entry(g, half) + half * 4 * HALF_ROWS
        target = lax.rem(chip + (15 if half == 0 else 1), 16)
        return remote(
            buf.at[pl.ds(here, HALF_ROWS), :],
            buf.at[pl.ds(there, HALF_ROWS), :],
            halo_send.at[g, half],
            halo_recv.at[g, half],
            "tm",
            target * 2 + core,
        )

    def hop(g, half, to):
        here = entry(g, half) + half * 4 * HALF_ROWS
        return remote(
            buf.at[pl.ds(here, HALF_ROWS), :],
            relay.at[pl.ds(g * HALF_ROWS, HALF_ROWS), :],
            halo_send.at[g, half],
            relay_recv.at[g],
            "tm",
            to,
        )

    def onward(g, half, to):
        there = entry(g, half) + (1 - half) * 4 * HALF_ROWS
        return remote(
            relay.at[pl.ds(g * HALF_ROWS, HALF_ROWS), :],
            buf.at[pl.ds(there, HALF_ROWS), :],
            relay_send.at[g],
            halo_recv.at[g, half],
            "tm",
            to,
        )

    relays = (core == 1) & ((x == 0) | (x == 3))
    relay_half = x // 3
    relay_to = device(z, 3 - x, core)

    def z_copy(g, way, step):
        near, far = partners(z, way)
        if step == 0:
            start, rows, into, to = (2 - keep(z, way)) * 32, 64, z_near, near
        else:
            start, rows, into, to = place(far, way) * 32, 32, z_far, far
        return remote(
            zs.at[way, g, pl.ds(start, rows), :],
            into.at[way, g],
            z_send.at[way, g, step],
            z_recv.at[way, g, step],
            "tm",
            device(to, x, core),
        )

    def x_copy(b, way, step):
        near, far = partners(x, way)
        if step == 0:
            start, size, into, to = 2 - keep(x, way), 2, x_near, near
        else:
            start, size, into, to = place(far, way), 1, x_far, far
        return remote(
            xs.at[way, b, pl.ds(start, size)],
            into.at[way, b],
            x_send.at[way, b, step],
            x_recv.at[way, b, step],
            "tm",
            device(z, to, core),
        )

    def d_copy(b, half, half_owner):
        rows = allf.at[half_owner, pl.ds(half * 192 + b * 32, 32), :]
        return remote(
            rows, rows, d_send.at[b, half], d_recv.at[b, half], "tm", device(z, x, other)
        )

    def edge_copy(stage, step):
        if stage == 0:
            return remote(
                edge_z.at[0], edge_z.at[step], e_send.at[0, step], e_recv.at[0, step],
                "tm", device(lax.rem(z + step, 4), x, core),
            )
        if stage == 1:
            return remote(
                edge_x.at[0], edge_x.at[step], e_send.at[1, step], e_recv.at[1, step],
                "tm", device(z, lax.rem(x + step, 4), core),
            )
        return remote(
            edge_sum.at[0], edge_sum.at[1], e_send.at[2, 0], e_recv.at[2, 0],
            "tm", device(z, x, other),
        )

    def mean_copy(step):
        target = core if step % 2 == 0 else other
        return remote(
            mean_buf.at[0], mean_buf.at[step], m_send.at[step], m_recv.at[step],
            "tm", device(z, x, target), chan=lax.rem(y + step // 2, 4),
        )

    def z_first(g):
        for way in range(2):
            z_copy(g, way, 0).start()

    def z_second(g):
        for way in range(2):
            far = partners(z, way)[1]
            z_copy(g, way, 0).wait_recv()
            at = place(far, way)
            rows = pl.ds(pl.multiple_of(at * 32, 32), 32)
            got = pl.ds(pl.multiple_of((at - keep(z, way)) * 32, 32), 32)
            zs[way, g, rows, :] = zs[way, g, rows, :] + z_near[way, g, got, :]
            z_copy(g, way, 1).start()

    def z_last(g):
        for way in range(2):
            z_copy(g, way, 1).wait_recv()
            at = place(z, way)
            rows = pl.ds(pl.multiple_of(at * 32, 32), 32)
            got = pl.ds(pl.multiple_of((at - keep(z, way)) * 32, 32), 32)
            total = zs[way, g, rows, :] + z_near[way, g, got, :] + z_far[way, g]
            for chunk in range(4):
                spot = (0, 2, 3, 1)[chunk] if way == 0 else chunk
                xs[way, g // 2, spot, lax.rem(g, 2)] = total[chunk * 8 : chunk * 8 + 8, :]

    def x_first(b):
        for way in range(2):
            x_copy(b, way, 0).start()

    def x_second(b):
        for way in range(2):
            far = partners(x, way)[1]
            x_copy(b, way, 0).wait_recv()
            at = place(far, way)
            xs[way, b, at] = xs[way, b, at] + x_near[way, b, at - keep(x, way)]
            x_copy(b, way, 1).start()

    def to_pair(b):
        for way in range(2):
            x_copy(b, way, 1).wait_recv()
            at = place(x, way)
            total = xs[way, b, at] + x_near[way, b, at - keep(x, way)] + x_far[way, b, 0]
            both = total[0] + total[1]
            mean_buf[0] = mean_buf[0] + (both[:, :ROOT] + both[:, ROOT:])
            for k in range(2):
                for i in range(2):
                    row = pl.multiple_of(k * 192 + b * 32 + (way * 2 + i) * 8, 8)
                    allf[core, pl.ds(row, 8), :] = total[k, :, i * ROOT : (i + 1) * ROOT]
        for k in range(2):
            d_copy(b, k, core).start()

        @pl.when(b == BATCHES - 1)
        def _():
            for s in range(1, 8):
                mean_copy(s).start()

    lane = lax.broadcasted_iota(jnp.int32, (8, ROOT), 1)
    sub = lax.broadcasted_iota(jnp.int32, (8, ROOT), 0)

    def phase(g, half, late):
        pair_index = (1 - half) if late else half
        first = pl.multiple_of(entry(g, half), 8)
        if late:
            halo(g, half).wait_recv()
        sums = []
        for i in range(2 * pair_index, 2 * pair_index + 3):
            rows = buf[pl.ds(pl.multiple_of(first + i * HALF_ROWS, 8), HALF_ROWS), :]
            rows = rows.reshape(64, 8, ROOT)
            sums.append(jnp.sum(jnp.sum(rows, axis=0), axis=1, keepdims=True))
        base = half * 32
        for i in range(2):
            mean = (sums[i] + sums[i + 1]) * (1.0 / SEG)
            at = base + (2 * pair_index + i) * 8
            mean_ref[at : at + 8, :] = jnp.broadcast_to(mean, (8, ROOT))
        mid_row = pl.multiple_of(g * 64 + base, 8)
        for ch in range(8):
            first_stage(
                buf, first, pair_index, ch, tabs, mean_ref, base, mid_ref, mid_row, high_ref, low_ref
            )
        gone = (chip == 15) if half == 0 else (chip == 0)
        for c0 in range(0, 8, CHUNK):
            sl = slice(c0 * 128, (c0 + CHUNK) * 128)
            sq = squares(high_ref[sl, :], low_ref[sl, :], tabs[1], tabs[2])
            for ch in range(c0, c0 + CHUNK):
                r = (ch - c0) * 128
                one, two = sq[r : r + 64], sq[r + 64 : r + 128]
                at = pl.multiple_of(g * 1024 + half * 512 + ch * 64, 64)
                if late:
                    if half == 0:
                        two = jnp.where(gone, 0.0, two)
                    else:
                        one = jnp.where(gone, 0.0, one)
                    pow_ref[pl.ds(at, 64), :] = pow_ref[pl.ds(at, 64), :] + (one + two)
                else:
                    pow_ref[pl.ds(at, 64), :] = one + two
        if not late:
            return
        sq = squares(*split(mid_ref[pl.ds(mid_row, 32), :]), tabs[1], tabs[2])
        middle = jnp.zeros((8, ROOT), F32)
        for s in range(SEGS):
            sqs = sq[s * 8 : s * 8 + 8]
            if s == 3 * (1 - half):
                sqs = jnp.where(gone, 0.0, sqs)
            middle = middle + sqs
        zeros = pl.ds(g * 1024 + half * 512, 8, 64)
        zero = pow_ref[zeros, :]
        last = jnp.sum(jnp.where(lane == ROOT - 1, zero, 0.0), axis=1, keepdims=True)
        spot = lane == 48 * half + 8 * g + sub
        edge_z[0] = jnp.where(spot, jnp.broadcast_to(last, (8, ROOT)), edge_z[0])
        pow_ref[zeros, :] = jnp.where(lax.rem(lane, 4) >= 2, middle, zero)
        for i in range(4):
            block = pow_ref[pl.ds(pl.multiple_of(g * 1024 + half * 512 + i * 128, 128), 128), :].T
            lanes = slice((i % 2) * ROOT, (i % 2 + 1) * ROOT)
            for chunk in range(4):
                spot = ((0, 2, 3, 1)[chunk] if i < 2 else chunk) * 32
                zs[i // 2, 2 * g + half, spot : spot + 32, lanes] = block[
                    chunk * 32 : chunk * 32 + 32
                ]

    def pair_arrival(g, half):
        to = entry(g, half) + (2 * other + half) * HALF_ROWS
        return remote(
            x_ref.at[pl.ds(0, 1024), :],
            buf.at[pl.ds(to, 1024), :],
            pair_send.at[g, half],
            pair_recv.at[g, half],
            "tm",
            device(z, x, other),
        )

    for g in range(GROUPS):
        for half in range(2):
            load(g, half).start()
    barrier = pltpu.get_barrier_semaphore()
    peers = [("tm", device(z, x, other))]
    for step in (1, 15):
        peers.append(("tm", lax.rem(chip + step, 16) * 2 + core))
    for step in (1, 3):
        peers.append(("tm", device(lax.rem(z + step, 4), x, core)))
        peers.append(("tm", device(z, lax.rem(x + step, 4), core)))
    peers.append(("tm", device(lax.rem(z + 2, 4), x, core)))
    peers.append(("tm", device(z, lax.rem(x + 2, 4), core)))
    signals = [{axis: index} for axis, index in peers]
    for step in (1, 2, 3):
        for to in (core, other):
            signals.append({"chan": lax.rem(y + step, 4), "tm": device(z, x, to)})
    for to in signals:
        pl.semaphore_signal(
            barrier, inc=1, device_id=to, device_id_type=pl.DeviceIdType.MESH
        )
    pl.semaphore_wait(barrier, len(signals))
    def arrived(g):
        for half in range(2):
            load(g, half).wait()
            pair_arrival(g, half).wait_recv()
            by_relay = (core == 1) & (x == 3 * half)
            to = device(lax.rem(z + 3 + 2 * half, 4), x, core)

            @pl.when(by_relay)
            def _():
                hop(g, half, to).start()

            @pl.when(jnp.logical_not(by_relay))
            def _():
                halo(g, half).start()

    def forward(g):
        @pl.when(relays)
        def _():
            hop(g, 0, relay_to).wait_recv()
            onward(g, relay_half, relay_to).start()

    for g in range(AHEAD + 1):
        for half in range(2):
            pair(g, half).start()
    edge_z[0] = jnp.zeros((8, ROOT), F32)
    mean_buf[0] = jnp.zeros((8, ROOT), F32)
    for g in range(AHEAD):
        arrived(g)
    for half in range(2):
        phase(0, half, False)
    forward(0)

    def step(g, carry):
        @pl.when(g < GROUPS - AHEAD - 1)
        def _():
            for half in range(2):
                pair(g + AHEAD + 1, half).start()

        @pl.when(g < GROUPS - AHEAD)
        def _():
            arrived(g + AHEAD)

        @pl.when(g < GROUPS - 1)
        def _():
            forward(g + 1)

        for half in range(2):
            entry_now = 2 * g + half

            @pl.when(g < GROUPS - 1)
            def _():
                phase(g + 1, half, False)

            @pl.when(g < GROUPS)
            def _():
                phase(g, half, True)
                z_first(entry_now)

            if half == 1:

                @pl.when(g == GROUPS - 1)
                def _():
                    for s in (1, 2, 3):
                        edge_copy(0, s).start()

            @pl.when((entry_now >= 2) & (entry_now < ENTRIES + 2))
            def _():
                z_second(entry_now - 2)

            @pl.when((entry_now >= 4) & (entry_now < ENTRIES + 4))
            def _():
                z_last(entry_now - 4)

            if half == 1:

                @pl.when((g >= 2) & (g < GROUPS + 2))
                def _():
                    x_first(g - 2)

                @pl.when((g >= 3) & (g < GROUPS + 3))
                def _():
                    x_second(g - 3)

                @pl.when(g >= 4)
                def _():
                    to_pair(g - 4)

        @pl.when(g == GROUPS)
        def _():
            total = edge_z[0]
            for s in (1, 2, 3):
                edge_copy(0, s).wait_recv()
                total = total + edge_z[s]
            edge_x[0] = total
            for s in (1, 2, 3):
                edge_copy(1, s).start()

        @pl.when(g == GROUPS + 1)
        def _():
            total = edge_x[0]
            for s in (1, 2, 3):
                edge_copy(1, s).wait_recv()
                total = total + edge_x[s]
            edge_sum[0] = total
            edge_copy(2, 0).start()

        return carry

    lax.fori_loop(0, GROUPS + 4, step, 0)
    for b in range(BATCHES):
        for k in range(2):
            d_copy(b, k, other).wait_recv()
    total = mean_buf[0]
    for s in range(1, 8):
        mean_copy(s).wait_recv()
        total = total + mean_buf[s]
    mean_sum[...] = total
    lane_row = lax.broadcasted_iota(jnp.int32, (1, ROOT), 1)
    for par in range(2):
        stacked = []
        for h in range(2):
            near = allf[h, pl.ds(4 * core + par, 48, 8), :]
            far = allf[h, pl.ds(4 * core + par + 2, 48, 8), :]
            stacked.append(jnp.concatenate([near, far], 1))
        row = jnp.concatenate(
            [mean_sum[pl.ds(4 * core + par, 1), :], mean_sum[pl.ds(4 * core + par + 2, 1), :]], 1
        )
        value = jnp.concatenate(stacked + [jnp.broadcast_to(row, (8, 256))], 0)
        high, rest = split(value)
        low = rest.astype(F32)
        rest = (value - high.astype(F32)) - low
        placed = dot(high, perm_ref[...]) + dot(low.astype(BF16), perm_ref[...])
        placed = placed + dot(rest.astype(BF16), perm_ref[...])
        factor = jnp.full((1, ROOT), 2.0 * scale, F32)
        if par == 0:
            factor = jnp.where((lane_row == 0) & (t == 0), scale, factor)
        for kind in range(2):
            out = placed[:, kind * ROOT : (kind + 1) * ROOT] * factor
            for h in range(2):
                for half in range(2):
                    at = h * 96 + half * 48 + kind
                    spread[par, pl.ds(at, 24, 2), :] = out[
                        h * 48 + half * 24 : h * 48 + half * 24 + 24
                    ]
        power_out[:, par * ROOT : (par + 1) * ROOT] = spread[par]
        row = (placed[96:97, :ROOT] + placed[96:97, ROOT:]) * factor
        mean_out[:, par * ROOT : (par + 1) * ROOT] = row * (1.0 / 768.0)

    def drain(g, carry):
        for way in range(2):
            for step in range(2):
                z_copy(2 * g, way, step).wait_send()
                z_copy(2 * g + 1, way, step).wait_send()
            pair(g, way).wait_send()
            halo(g, way).wait_send()

        @pl.when(relays)
        def _():
            onward(g, relay_half, relay_to).wait_send()

        return carry

    lax.fori_loop(0, GROUPS, drain, 0)
    for b in range(BATCHES):
        for way in range(2):
            for step in range(2):
                x_copy(b, way, step).wait_send()
        for k in range(2):
            d_copy(b, k, core).wait_send()
    for s in (1, 2, 3):
        edge_copy(0, s).wait_send()
        edge_copy(1, s).wait_send()
    edge_copy(2, 0).wait_recv()
    edge_copy(2, 0).wait_send()
    for h in range(2):
        mine = jnp.where(core == h, edge_sum[0], edge_sum[1])
        row = jnp.sum(mine, axis=0, keepdims=True) * scale
        edge_out[:, h * 96 : h * 96 + 96] = row[:, :96]
    for s in range(1, 8):
        mean_copy(s).wait_send()


def per_device(strain):
    rows = strain.shape[0]
    tabs_np, energy = tables()
    tabs = [jnp.asarray(t) for t in tabs_np]
    groups = rows // 8
    x4 = strain.reshape(groups, 8, ROOT, ROOT).transpose(0, 2, 1, 3)
    x2 = x4.reshape(groups * 1024, ROOT)
    vmem = pl.BlockSpec(memory_space=pltpu.VMEM)
    dma = pltpu.SemaphoreType.DMA
    power, edge, mean = pl.pallas_call(
        functools.partial(welch_kernel, 1.0 / (63.0 * energy)),
        out_shape=[
            jax.ShapeDtypeStruct((192, 256), F32),
            jax.ShapeDtypeStruct((1, 192), F32),
            jax.ShapeDtypeStruct((1, 256), F32),
        ],
        in_specs=[pl.BlockSpec(memory_space=pl.ANY)] + [vmem] * len(tabs),
        out_specs=[vmem] * 3,
        scratch_shapes=[
            pltpu.VMEM((GROUPS * HALF_ROWS, ROOT), F32),
            dma((GROUPS,)),
            dma((GROUPS,)),
            pltpu.VMEM((2, 192, ROOT), F32),
            pltpu.VMEM((GROUPS * 2 * ENTRY_ROWS, ROOT), F32),
            pltpu.VMEM((64, ROOT), F32),
            pltpu.VMEM((GROUPS * 64, 256), F32),
            pltpu.VMEM((1024, 256), BF16),
            pltpu.VMEM((1024, 256), BF16),
            pltpu.VMEM((GROUPS * 1024, ROOT), F32),
            pltpu.VMEM((2, ENTRIES, 128, 256), F32),
            pltpu.VMEM((2, ENTRIES, 64, 256), F32),
            pltpu.VMEM((2, ENTRIES, 32, 256), F32),
            pltpu.VMEM((2, BATCHES, 4, 2, 8, 256), F32),
            pltpu.VMEM((2, BATCHES, 2, 2, 8, 256), F32),
            pltpu.VMEM((2, BATCHES, 1, 2, 8, 256), F32),
            pltpu.VMEM((2, GROUPS * 64, ROOT), F32),
            pltpu.VMEM((4, 8, ROOT), F32),
            pltpu.VMEM((4, 8, ROOT), F32),
            pltpu.VMEM((2, 8, ROOT), F32),
            pltpu.VMEM((8, 8, ROOT), F32),
            pltpu.VMEM((8, ROOT), F32),
            dma((GROUPS, 2)),
            dma((GROUPS, 2)),
            dma((GROUPS, 2)),
            dma((GROUPS, 2)),
            dma((GROUPS, 2)),
            dma((2, ENTRIES, 2)),
            dma((2, ENTRIES, 2)),
            dma((2, BATCHES, 2)),
            dma((2, BATCHES, 2)),
            dma((BATCHES, 2)),
            dma((BATCHES, 2)),
            dma((3, 4)),
            dma((3, 4)),
            dma((8,)),
            dma((8,)),
        ],
        compiler_params=pltpu.CompilerParams(
            collective_id=0, has_side_effects=True, vmem_limit_bytes=60 * 1024 * 1024
        ),
    )(x2, *tabs)
    nyquist = edge.reshape(rows)
    return power, nyquist, mean.reshape(256)


def solution(mesh):
    return jax.shard_map(
        per_device,
        mesh=mesh,
        in_specs=(P("chan", "tm"),),
        out_specs=(P("chan", "tm"), P("chan"), P("tm")),
        check_vma=False,
    )
```

```python
import functools

import jax
import jax.numpy as jnp
import numpy as np
from jax import lax
from jax.experimental import pallas as pl
from jax.experimental.pallas import tpu as pltpu
from jax.sharding import PartitionSpec as P

SEG = 16384
ROOT = 128
F32 = jnp.float32
BF16 = jnp.bfloat16
STRIDE = 8
CHUNK = 8


def split(values):
    high = values.astype(BF16)
    low = (values - high.astype(F32)).astype(BF16)
    return high, low


def split_np(values):
    high = values.astype(np.float32).astype(BF16)
    low = (values - high.astype(np.float64)).astype(np.float32).astype(BF16)
    return high, low


def lane_bins():
    lane = np.arange(ROOT)
    owner, part = lane // 4, lane % 4
    return np.where(part < 2, 2 * owner + part, 127 - 2 * owner - (part - 2))


def tables():
    turn = 2.0 * np.pi / ROOT
    a = np.arange(ROOT)
    k1 = np.arange(64)
    cos_rows = np.cos(turn * ((k1[:, None] * a) % ROOT))
    sin_rows = -np.sin(turn * ((k1[:, None] * a) % ROOT))
    sin_rows[0] = 1.0 - 2.0 * (a % 2)
    first = np.concatenate([cos_rows, sin_rows], 0)
    first_high, first_low = split_np(first)
    first_high = np.concatenate([first_high, first_high], 1)
    first_low = np.concatenate([first_low, first_low], 1)
    q = lane_bins()
    cos_q = np.cos(turn * ((a[:, None] * q) % ROOT))
    sin_q = np.sin(turn * ((a[:, None] * q) % ROOT))
    last = np.concatenate(
        [np.concatenate([cos_q, -sin_q], 1), np.concatenate([sin_q, cos_q], 1)], 0
    )
    last_high, last_low = split_np(last)
    long_turn = 2.0 * np.pi / SEG
    twist = long_turn * (k1[:, None] * a)
    cos_twist = np.cos(twist).astype(np.float32)
    sin_twist = np.sin(twist).astype(np.float32)
    mid = long_turn * 64 * a
    mid_twist = np.stack([np.cos(mid), np.sin(mid)] + [0 * mid] * 6).astype(np.float32)
    n = np.arange(SEG, dtype=np.float64)
    window = (0.5 - 0.5 * np.cos(2.0 * np.pi * n / SEG)).astype(np.float32)
    slot, kind, k = np.meshgrid(np.arange(2), np.arange(2), np.arange(64), indexing="ij")
    place = np.where(slot == 0, k, np.where(k == 0, 64, 128 - k)) + 128 * kind
    perm = np.zeros((256, 256), np.float32)
    perm[np.arange(256), place.reshape(-1)] = 1.0
    energy = float(np.sum(window.astype(np.float64) ** 2))
    return (
        [
            np.concatenate([first_high, first_low], 0),
            last_high,
            last_low,
            cos_twist,
            sin_twist,
            mid_twist,
            window.reshape(ROOT, ROOT),
            perm.astype(BF16),
        ],
        energy,
    )


def dot(a, b):
    return jnp.dot(a, b, preferred_element_type=F32)


def first_stage(blocks, start, pair, ch, tabs, mean_ref, mean_base, mid_ref, mid_row, high_ref, low_ref):
    t_ref, vh_ref, vl_ref, c_ref, s_ref, mid_tw, w_ref = tabs
    w0, w1 = w_ref[:64, :], w_ref[64:, :]
    row = lax.broadcasted_iota(jnp.int32, (8, 256), 0)
    highs, lows = [], []
    for s in (2 * pair, 2 * pair + 1):
        mean = mean_ref[pl.ds(mean_base + s * 8 + ch, 1), :]
        r0, b0, b1 = blocks, start + s * 512, start + s * 512 + 512
        x0 = (r0[pl.ds(b0 + ch, 64, STRIDE), :] - mean) * w0
        x1 = (r0[pl.ds(b1 + ch, 64, STRIDE), :] - mean) * w1
        high, low = split(jnp.concatenate([x0, x1], 0))
        highs.append(high)
        lows.append(low)
    x = jnp.concatenate(
        [jnp.concatenate(highs, 1), jnp.concatenate(lows, 1)], 0
    )
    both = dot(t_ref[...], x)
    d = both[:128] + both[128:]
    fr = d[:64]
    fi = jnp.concatenate([jnp.where(row == 0, 0.0, d[64:72]), d[72:]], 0)
    mid = d[64:65]
    c, s_ = c_ref[...], s_ref[...]
    for i in range(2):
        s = 2 * pair + i
        lanes = slice(i * ROOT, (i + 1) * ROOT)
        tr = fr[:, lanes] * c + fi[:, lanes] * s_
        ti = fi[:, lanes] * c - fr[:, lanes] * s_
        put = ch * 128 + 64 * i
        high, low = split(jnp.concatenate([tr, ti], 1))
        high_ref[pl.ds(put, 64), :] = high
        low_ref[pl.ds(put, 64), :] = low
        m = mid[:, lanes]
        mid_ref[pl.ds(mid_row + s * 8 + ch, 1), :] = jnp.concatenate(
            [m * mid_tw[0:1, :], -m * mid_tw[1:2, :]], 1
        )


def squares(high, low, vh_ref, vl_ref):
    o = dot(high, vh_ref[...]) + dot(low, vh_ref[...]) + dot(high, vl_ref[...])
    return o[:, :ROOT] * o[:, :ROOT] + o[:, ROOT:] * o[:, ROOT:]


GROUPS = 6
HALF_ROWS = 512
ENTRY_ROWS = 5 * HALF_ROWS
SEGS = 4
ENTRIES = 2 * GROUPS
BATCHES = GROUPS
AHEAD = 2


def remote(src, dst, send, recv, axis, index, **more):
    return pltpu.make_async_remote_copy(
        src_ref=src,
        dst_ref=dst,
        send_sem=send,
        recv_sem=recv,
        device_id={axis: index, **more},
        device_id_type=pl.DeviceIdType.MESH,
    )


def twin(r):
    return r + 1 - 2 * lax.rem(r, 2)


def partners(r, way):
    if way == 0:
        return twin(r), 3 - r
    return 3 - r, twin(r)


def place(r, way):
    if way == 0:
        return lax.rem(2 * r - r // 2, 4)
    return r


def keep(r, way):
    return place(r, way) // 2 * 2


def welch_kernel(scale, x_ref, *refs):
    tabs, perm_ref, refs = refs[:7], refs[7], refs[8:]
    power_out, edge_out, mean_out = refs[:3]
    (relay, relay_send, relay_recv, spread), refs = refs[3:7], refs[:3] + refs[7:]
    (buf, mean_ref, mid_ref, high_ref, low_ref, pow_ref) = refs[3:9]
    (zs, z_near, z_far, xs, x_near, x_far, allf) = refs[9:16]
    (edge_z, edge_x, edge_sum, mean_buf, mean_sum), refs = refs[16:21], refs[:20] + refs[21:]
    (load_sem, pair_send, pair_recv, halo_send, halo_recv, z_send, z_recv) = refs[20:27]
    (x_send, x_recv, d_send, d_recv, e_send, e_recv, m_send, m_recv) = refs[27:]
    y = lax.axis_index("chan")
    t = lax.axis_index("tm")
    core = lax.rem(t, 2)
    chip = t // 2
    x = lax.rem(chip, 4)
    z = chip // 4
    other = 1 - core
    device = lambda zz, xx, cc: (zz * 4 + xx) * 2 + cc

    def entry(g, half):
        return (g * 2 + half) * ENTRY_ROWS

    def load(g, half):
        row = (12 * core + 6 * half + g) * 1024
        to = entry(g, half) + (2 * core + half) * HALF_ROWS
        return pltpu.make_async_copy(
            x_ref.at[pl.ds(row, 1024), :], buf.at[pl.ds(to, 1024), :], load_sem.at[g, half]
        )

    def pair(g, half):
        row = (12 * other + 6 * half + g) * 1024
        to = entry(g, half) + (2 * core + half) * HALF_ROWS
        return remote(
            x_ref.at[pl.ds(row, 1024), :],
            buf.at[pl.ds(to, 1024), :],
            pair_send.at[g, half],
            pair_recv.at[g, half],
            "tm",
            device(z, x, other),
        )

    def halo(g, half):
        there = entry(g, half) + (1 - half) * 4 * HALF_ROWS
        here = entry(g, half) + half * 4 * HALF_ROWS
        target = lax.rem(chip + (15 if half == 0 else 1), 16)
        return remote(
            buf.at[pl.ds(here, HALF_ROWS), :],
            buf.at[pl.ds(there, HALF_ROWS), :],
            halo_send.at[g, half],
            halo_recv.at[g, half],
            "tm",
            target * 2 + core,
        )

    def hop(g, half, to):
        here = entry(g, half) + half * 4 * HALF_ROWS
        return remote(
            buf.at[pl.ds(here, HALF_ROWS), :],
            relay.at[pl.ds(g * HALF_ROWS, HALF_ROWS), :],
            halo_send.at[g, half],
            relay_recv.at[g],
            "tm",
            to,
        )

    def onward(g, half, to):
        there = entry(g, half) + (1 - half) * 4 * HALF_ROWS
        return remote(
            relay.at[pl.ds(g * HALF_ROWS, HALF_ROWS), :],
            buf.at[pl.ds(there, HALF_ROWS), :],
            relay_send.at[g],
            halo_recv.at[g, half],
            "tm",
            to,
        )

    relays = (core == 1) & ((x == 0) | (x == 3))
    relay_half = x // 3
    relay_to = device(z, 3 - x, core)

    def z_copy(g, way, step):
        near, far = partners(z, way)
        if step == 0:
            start, rows, into, to = (2 - keep(z, way)) * 32, 64, z_near, near
        else:
            start, rows, into, to = place(far, way) * 32, 32, z_far, far
        return remote(
            zs.at[way, g, pl.ds(start, rows), :],
            into.at[way, g],
            z_send.at[way, g, step],
            z_recv.at[way, g, step],
            "tm",
            device(to, x, core),
        )

    def x_copy(b, way, step):
        near, far = partners(x, way)
        if step == 0:
            start, size, into, to = 2 - keep(x, way), 2, x_near, near
        else:
            start, size, into, to = place(far, way), 1, x_far, far
        return remote(
            xs.at[way, b, pl.ds(start, size)],
            into.at[way, b],
            x_send.at[way, b, step],
            x_recv.at[way, b, step],
            "tm",
            device(z, to, core),
        )

    def d_copy(b, half, half_owner):
        rows = allf.at[half_owner, pl.ds(half * 192 + b * 32, 32), :]
        return remote(
            rows, rows, d_send.at[b, half], d_recv.at[b, half], "tm", device(z, x, other)
        )

    def edge_copy(stage, step):
        if stage == 0:
            return remote(
                edge_z.at[0], edge_z.at[step], e_send.at[0, step], e_recv.at[0, step],
                "tm", device(lax.rem(z + step, 4), x, core),
            )
        if stage == 1:
            return remote(
                edge_x.at[0], edge_x.at[step], e_send.at[1, step], e_recv.at[1, step],
                "tm", device(z, lax.rem(x + step, 4), core),
            )
        return remote(
            edge_sum.at[0], edge_sum.at[1], e_send.at[2, 0], e_recv.at[2, 0],
            "tm", device(z, x, other),
        )

    def mean_copy(step):
        target = core if step % 2 == 0 else other
        return remote(
            mean_buf.at[0], mean_buf.at[step], m_send.at[step], m_recv.at[step],
            "tm", device(z, x, target), chan=lax.rem(y + step // 2, 4),
        )

    def z_first(g):
        for way in range(2):
            z_copy(g, way, 0).start()

    def z_second(g):
        for way in range(2):
            far = partners(z, way)[1]
            z_copy(g, way, 0).wait_recv()
            at = place(far, way)
            rows = pl.ds(pl.multiple_of(at * 32, 32), 32)
            got = pl.ds(pl.multiple_of((at - keep(z, way)) * 32, 32), 32)
            zs[way, g, rows, :] = zs[way, g, rows, :] + z_near[way, g, got, :]
            z_copy(g, way, 1).start()

    def z_last(g):
        for way in range(2):
            z_copy(g, way, 1).wait_recv()
            at = place(z, way)
            rows = pl.ds(pl.multiple_of(at * 32, 32), 32)
            got = pl.ds(pl.multiple_of((at - keep(z, way)) * 32, 32), 32)
            total = zs[way, g, rows, :] + z_near[way, g, got, :] + z_far[way, g]
            for chunk in range(4):
                spot = (0, 2, 3, 1)[chunk] if way == 0 else chunk
                xs[way, g // 2, spot, lax.rem(g, 2)] = total[chunk * 8 : chunk * 8 + 8, :]

    def x_first(b):
        for way in range(2):
            x_copy(b, way, 0).start()

    def x_second(b):
        for way in range(2):
            far = partners(x, way)[1]
            x_copy(b, way, 0).wait_recv()
            at = place(far, way)
            xs[way, b, at] = xs[way, b, at] + x_near[way, b, at - keep(x, way)]
            x_copy(b, way, 1).start()

    def to_pair(b):
        for way in range(2):
            x_copy(b, way, 1).wait_recv()
            at = place(x, way)
            total = xs[way, b, at] + x_near[way, b, at - keep(x, way)] + x_far[way, b, 0]
            both = total[0] + total[1]
            mean_buf[0] = mean_buf[0] + (both[:, :ROOT] + both[:, ROOT:])
            for k in range(2):
                for i in range(2):
                    row = pl.multiple_of(k * 192 + b * 32 + (way * 2 + i) * 8, 8)
                    allf[core, pl.ds(row, 8), :] = total[k, :, i * ROOT : (i + 1) * ROOT]
        for k in range(2):
            d_copy(b, k, core).start()

        @pl.when(b == BATCHES - 1)
        def _():
            for s in range(1, 8):
                mean_copy(s).start()

    lane = lax.broadcasted_iota(jnp.int32, (8, ROOT), 1)
    sub = lax.broadcasted_iota(jnp.int32, (8, ROOT), 0)

    def phase(g, half, late):
        pair_index = (1 - half) if late else half
        first = pl.multiple_of(entry(g, half), 8)
        if late:
            halo(g, half).wait_recv()
        sums = []
        for i in range(2 * pair_index, 2 * pair_index + 3):
            rows = buf[pl.ds(pl.multiple_of(first + i * HALF_ROWS, 8), HALF_ROWS), :]
            rows = rows.reshape(64, 8, ROOT)
            sums.append(jnp.sum(jnp.sum(rows, axis=0), axis=1, keepdims=True))
        base = half * 32
        for i in range(2):
            mean = (sums[i] + sums[i + 1]) * (1.0 / SEG)
            at = base + (2 * pair_index + i) * 8
            mean_ref[at : at + 8, :] = jnp.broadcast_to(mean, (8, ROOT))
        mid_row = pl.multiple_of(g * 64 + base, 8)
        for ch in range(8):
            first_stage(
                buf, first, pair_index, ch, tabs, mean_ref, base, mid_ref, mid_row, high_ref, low_ref
            )
        gone = (chip == 15) if half == 0 else (chip == 0)
        for c0 in range(0, 8, CHUNK):
            sl = slice(c0 * 128, (c0 + CHUNK) * 128)
            sq = squares(high_ref[sl, :], low_ref[sl, :], tabs[1], tabs[2])
            for ch in range(c0, c0 + CHUNK):
                r = (ch - c0) * 128
                one, two = sq[r : r + 64], sq[r + 64 : r + 128]
                at = pl.multiple_of(g * 1024 + half * 512 + ch * 64, 64)
                if late:
                    if half == 0:
                        two = jnp.where(gone, 0.0, two)
                    else:
                        one = jnp.where(gone, 0.0, one)
                    pow_ref[pl.ds(at, 64), :] = pow_ref[pl.ds(at, 64), :] + (one + two)
                else:
                    pow_ref[pl.ds(at, 64), :] = one + two
        if not late:
            return
        sq = squares(*split(mid_ref[pl.ds(mid_row, 32), :]), tabs[1], tabs[2])
        middle = jnp.zeros((8, ROOT), F32)
        for s in range(SEGS):
            sqs = sq[s * 8 : s * 8 + 8]
            if s == 3 * (1 - half):
                sqs = jnp.where(gone, 0.0, sqs)
            middle = middle + sqs
        zeros = pl.ds(g * 1024 + half * 512, 8, 64)
        zero = pow_ref[zeros, :]
        last = jnp.sum(jnp.where(lane == ROOT - 1, zero, 0.0), axis=1, keepdims=True)
        spot = lane == 48 * half + 8 * g + sub
        edge_z[0] = jnp.where(spot, jnp.broadcast_to(last, (8, ROOT)), edge_z[0])
        pow_ref[zeros, :] = jnp.where(lax.rem(lane, 4) >= 2, middle, zero)
        for i in range(4):
            block = pow_ref[pl.ds(pl.multiple_of(g * 1024 + half * 512 + i * 128, 128), 128), :].T
            lanes = slice((i % 2) * ROOT, (i % 2 + 1) * ROOT)
            for chunk in range(4):
                spot = ((0, 2, 3, 1)[chunk] if i < 2 else chunk) * 32
                zs[i // 2, 2 * g + half, spot : spot + 32, lanes] = block[
                    chunk * 32 : chunk * 32 + 32
                ]

    def pair_arrival(g, half):
        to = entry(g, half) + (2 * other + half) * HALF_ROWS
        return remote(
            x_ref.at[pl.ds(0, 1024), :],
            buf.at[pl.ds(to, 1024), :],
            pair_send.at[g, half],
            pair_recv.at[g, half],
            "tm",
            device(z, x, other),
        )

    for g in range(GROUPS):
        for half in range(2):
            load(g, half).start()
    barrier = pltpu.get_barrier_semaphore()
    peers = [("tm", device(z, x, other))]
    for step in (1, 15):
        peers.append(("tm", lax.rem(chip + step, 16) * 2 + core))
    for step in (1, 3):
        peers.append(("tm", device(lax.rem(z + step, 4), x, core)))
        peers.append(("tm", device(z, lax.rem(x + step, 4), core)))
    peers.append(("tm", device(lax.rem(z + 2, 4), x, core)))
    peers.append(("tm", device(z, lax.rem(x + 2, 4), core)))
    signals = [{axis: index} for axis, index in peers]
    for step in (1, 2, 3):
        for to in (core, other):
            signals.append({"chan": lax.rem(y + step, 4), "tm": device(z, x, to)})
    for to in signals:
        pl.semaphore_signal(
            barrier, inc=1, device_id=to, device_id_type=pl.DeviceIdType.MESH
        )
    pl.semaphore_wait(barrier, len(signals))
    def arrived(g):
        for half in range(2):
            load(g, half).wait()
            pair_arrival(g, half).wait_recv()
            by_relay = (core == 1) & (x == 3 * half)
            to = device(lax.rem(z + 3 + 2 * half, 4), x, core)

            @pl.when(by_relay)
            def _():
                hop(g, half, to).start()

            @pl.when(jnp.logical_not(by_relay))
            def _():
                halo(g, half).start()

    def forward(g):
        @pl.when(relays)
        def _():
            hop(g, 0, relay_to).wait_recv()
            onward(g, relay_half, relay_to).start()

    for g in range(AHEAD + 1):
        for half in range(2):
            pair(g, half).start()
    edge_z[0] = jnp.zeros((8, ROOT), F32)
    mean_buf[0] = jnp.zeros((8, ROOT), F32)
    for g in range(AHEAD):
        arrived(g)
    for half in range(2):
        phase(0, half, False)
    forward(0)

    def step(g, carry):
        @pl.when(g < GROUPS - AHEAD - 1)
        def _():
            for half in range(2):
                pair(g + AHEAD + 1, half).start()

        @pl.when(g < GROUPS - AHEAD)
        def _():
            arrived(g + AHEAD)

        for half in range(2):
            entry_now = 2 * g + half

            @pl.when(g < GROUPS - 1)
            def _():
                phase(g + 1, half, False)

            if half == 0:

                @pl.when(g < GROUPS - 1)
                def _():
                    forward(g + 1)

            @pl.when(g < GROUPS)
            def _():
                phase(g, half, True)
                z_first(entry_now)

            if half == 1:

                @pl.when(g == GROUPS - 1)
                def _():
                    for s in (1, 2, 3):
                        edge_copy(0, s).start()

            @pl.when((entry_now >= 2) & (entry_now < ENTRIES + 2))
            def _():
                z_second(entry_now - 2)

            @pl.when((entry_now >= 4) & (entry_now < ENTRIES + 4))
            def _():
                z_last(entry_now - 4)

            if half == 1:

                @pl.when((g >= 2) & (g < GROUPS + 2))
                def _():
                    x_first(g - 2)

                @pl.when((g >= 3) & (g < GROUPS + 3))
                def _():
                    x_second(g - 3)

                @pl.when(g >= 4)
                def _():
                    to_pair(g - 4)

        @pl.when(g == GROUPS)
        def _():
            total = edge_z[0]
            for s in (1, 2, 3):
                edge_copy(0, s).wait_recv()
                total = total + edge_z[s]
            edge_x[0] = total
            for s in (1, 2, 3):
                edge_copy(1, s).start()

        @pl.when(g == GROUPS + 1)
        def _():
            total = edge_x[0]
            for s in (1, 2, 3):
                edge_copy(1, s).wait_recv()
                total = total + edge_x[s]
            edge_sum[0] = total
            edge_copy(2, 0).start()

        return carry

    lax.fori_loop(0, GROUPS + 4, step, 0)
    for b in range(BATCHES):
        for k in range(2):
            d_copy(b, k, other).wait_recv()
    total = mean_buf[0]
    for s in range(1, 8):
        mean_copy(s).wait_recv()
        total = total + mean_buf[s]
    mean_sum[...] = total
    lane_row = lax.broadcasted_iota(jnp.int32, (1, ROOT), 1)
    for par in range(2):
        stacked = []
        for h in range(2):
            near = allf[h, pl.ds(4 * core + par, 48, 8), :]
            far = allf[h, pl.ds(4 * core + par + 2, 48, 8), :]
            stacked.append(jnp.concatenate([near, far], 1))
        row = jnp.concatenate(
            [mean_sum[pl.ds(4 * core + par, 1), :], mean_sum[pl.ds(4 * core + par + 2, 1), :]], 1
        )
        value = jnp.concatenate(stacked + [jnp.broadcast_to(row, (8, 256))], 0)
        high, rest = split(value)
        low = rest.astype(F32)
        rest = (value - high.astype(F32)) - low
        placed = dot(high, perm_ref[...]) + dot(low.astype(BF16), perm_ref[...])
        placed = placed + dot(rest.astype(BF16), perm_ref[...])
        factor = jnp.full((1, ROOT), 2.0 * scale, F32)
        if par == 0:
            factor = jnp.where((lane_row == 0) & (t == 0), scale, factor)
        for kind in range(2):
            out = placed[:, kind * ROOT : (kind + 1) * ROOT] * factor
            for h in range(2):
                for half in range(2):
                    at = h * 96 + half * 48 + kind
                    spread[par, pl.ds(at, 24, 2), :] = out[
                        h * 48 + half * 24 : h * 48 + half * 24 + 24
                    ]
        power_out[:, par * ROOT : (par + 1) * ROOT] = spread[par]
        row = (placed[96:97, :ROOT] + placed[96:97, ROOT:]) * factor
        mean_out[:, par * ROOT : (par + 1) * ROOT] = row * (1.0 / 768.0)

    def drain(g, carry):
        for way in range(2):
            for step in range(2):
                z_copy(2 * g, way, step).wait_send()
                z_copy(2 * g + 1, way, step).wait_send()
            pair(g, way).wait_send()
            halo(g, way).wait_send()

        @pl.when(relays)
        def _():
            onward(g, relay_half, relay_to).wait_send()

        return carry

    lax.fori_loop(0, GROUPS, drain, 0)
    for b in range(BATCHES):
        for way in range(2):
            for step in range(2):
                x_copy(b, way, step).wait_send()
        for k in range(2):
            d_copy(b, k, core).wait_send()
    for s in (1, 2, 3):
        edge_copy(0, s).wait_send()
        edge_copy(1, s).wait_send()
    edge_copy(2, 0).wait_recv()
    edge_copy(2, 0).wait_send()
    for h in range(2):
        mine = jnp.where(core == h, edge_sum[0], edge_sum[1])
        row = jnp.sum(mine, axis=0, keepdims=True) * scale
        edge_out[:, h * 96 : h * 96 + 96] = row[:, :96]
    for s in range(1, 8):
        mean_copy(s).wait_send()


def per_device(strain):
    rows = strain.shape[0]
    tabs_np, energy = tables()
    tabs = [jnp.asarray(t) for t in tabs_np]
    groups = rows // 8
    x4 = strain.reshape(groups, 8, ROOT, ROOT).transpose(0, 2, 1, 3)
    x2 = x4.reshape(groups * 1024, ROOT)
    vmem = pl.BlockSpec(memory_space=pltpu.VMEM)
    dma = pltpu.SemaphoreType.DMA
    power, edge, mean = pl.pallas_call(
        functools.partial(welch_kernel, 1.0 / (63.0 * energy)),
        out_shape=[
            jax.ShapeDtypeStruct((192, 256), F32),
            jax.ShapeDtypeStruct((1, 192), F32),
            jax.ShapeDtypeStruct((1, 256), F32),
        ],
        in_specs=[pl.BlockSpec(memory_space=pl.ANY)] + [vmem] * len(tabs),
        out_specs=[vmem] * 3,
        scratch_shapes=[
            pltpu.VMEM((GROUPS * HALF_ROWS, ROOT), F32),
            dma((GROUPS,)),
            dma((GROUPS,)),
            pltpu.VMEM((2, 192, ROOT), F32),
            pltpu.VMEM((GROUPS * 2 * ENTRY_ROWS, ROOT), F32),
            pltpu.VMEM((64, ROOT), F32),
            pltpu.VMEM((GROUPS * 64, 256), F32),
            pltpu.VMEM((1024, 256), BF16),
            pltpu.VMEM((1024, 256), BF16),
            pltpu.VMEM((GROUPS * 1024, ROOT), F32),
            pltpu.VMEM((2, ENTRIES, 128, 256), F32),
            pltpu.VMEM((2, ENTRIES, 64, 256), F32),
            pltpu.VMEM((2, ENTRIES, 32, 256), F32),
            pltpu.VMEM((2, BATCHES, 4, 2, 8, 256), F32),
            pltpu.VMEM((2, BATCHES, 2, 2, 8, 256), F32),
            pltpu.VMEM((2, BATCHES, 1, 2, 8, 256), F32),
            pltpu.VMEM((2, GROUPS * 64, ROOT), F32),
            pltpu.VMEM((4, 8, ROOT), F32),
            pltpu.VMEM((4, 8, ROOT), F32),
            pltpu.VMEM((2, 8, ROOT), F32),
            pltpu.VMEM((8, 8, ROOT), F32),
            pltpu.VMEM((8, ROOT), F32),
            dma((GROUPS, 2)),
            dma((GROUPS, 2)),
            dma((GROUPS, 2)),
            dma((GROUPS, 2)),
            dma((GROUPS, 2)),
            dma((2, ENTRIES, 2)),
            dma((2, ENTRIES, 2)),
            dma((2, BATCHES, 2)),
            dma((2, BATCHES, 2)),
            dma((BATCHES, 2)),
            dma((BATCHES, 2)),
            dma((3, 4)),
            dma((3, 4)),
            dma((8,)),
            dma((8,)),
        ],
        compiler_params=pltpu.CompilerParams(
            collective_id=0, has_side_effects=True, vmem_limit_bytes=60 * 1024 * 1024
        ),
    )(x2, *tabs)
    nyquist = edge.reshape(rows)
    return power, nyquist, mean.reshape(256)


def solution(mesh):
    return jax.shard_map(
        per_device,
        mesh=mesh,
        in_specs=(P("chan", "tm"),),
        out_specs=(P("chan", "tm"), P("chan"), P("tm")),
        check_vma=False,
    )
```
